128 devices in a mesh: section: 8 (over x, core), expert: 4 (over y), dp: 4 (over z).
Axes of the slice: x: 4, y: 4, z: 4, core: 2. Of those that a mesh axis runs over, the one named last changes fastest.
Arguments:
- x_in: bfloat16 [8, 256, 2048], P(None, ('expert', 'dp'), 'section'), may hold values from -6 to 6
- cotangent: bfloat16 [8, 256, 2048], P(None, ('expert', 'dp'), 'section'), may hold values from -6 to 6
- route_ids: int32 [8, 8, 256, 2], P('section', None, ('expert', 'dp')), may hold values from 0 to 15, all different within a row; in each aligned block of 16 rows (0 to 15, 16 to 31, ..., all dimensions but the last counted through in order) at most 2 rows name the same one
- norm_gain: float32 [8, 2048], P('section'), may hold values from 0.5 to 1.5
- router: bfloat16 [8, 2048, 16], P('section'), may hold values from -0.125 to 0.125
- w_gate_up: bfloat16 [8, 16, 2048, 1024], P('section', ('expert', 'dp')), may hold values from -0.125 to 0.125
- w_down: bfloat16 [8, 16, 512, 2048], P('section', ('expert', 'dp')), may hold values from -0.25 to 0.25
Outputs:
- grad_in: bfloat16 [8, 256, 2048], P(None, ('expert', 'dp'), 'section')
- grad_gate_up: float32 [8, 16, 2048, 1024], P('section', ('expert', 'dp'))
- grad_down: float32 [8, 16, 512, 2048], P('section', ('expert', 'dp'))
- grad_router: float32 [8, 2048, 16], P('section')
- grad_gain: float32 [8, 2048], P('section')
The draws below stay inside these ranges and needn't reach their ends.
Inputs may be any that keep to these rules, and one draw needn't show every extreme that they name: `route_ids`: each row names two different experts; the 16 rows of one device in one layer and micro-batch name any expert at most 2 times, a bound that some block reaches in some of them.
All inputs are finite; a program needn't handle non-finite values.
Results may differ from the reference program's by a relative error of at most 0.035.
Values may be sent and summed in bfloat16 or wider, within the bound.
A program may use at most 64 MiB of HBM per device.

```python
import math
import jax
import jax.numpy as jnp
import numpy as np
from jax import lax

D = 2048
FFW = 512
TOP = 2
MICRO = 8
TOK_DEV = 16
EXPERTS = 16
CAP = 2
ROWS = 256
SECTIONS = 8


def shard_levels(own_key, shape, pieces, low, high):
    def one(axis_at, blocks):
        heights = jax.random.uniform(jax.random.fold_in(jax.random.fold_in(own_key, 6), axis_at), (blocks,), jnp.float32, low / len(pieces), high / len(pieces))
        return jnp.repeat(jnp.exp(heights), shape[axis_at] // blocks).reshape((-1,) + (1,) * (len(shape) - axis_at - 1))

    level = one(*pieces[0])
    for cut in pieces[1:]:
        level = level * one(*cut)
    return level


def routed_block(key, own, number, rows, count, top, reach, lean):
    sequence = jax.random.permutation(key, count)
    packed, ordinary = shares(count, rows * top, reach, lean, True), shares(count, rows * top, reach, lean, False)
    places = jnp.arange(count)

    def named(lengths, turn):
        used = int((lengths > 0).sum())
        fixed = max(1, used // 4)
        moved = fixed + (places - fixed + turn * (used - fixed)) % max(1, count - fixed)
        return jnp.zeros((count,), jnp.int32).at[sequence[jnp.where(places < fixed, places, moved)]].set(jnp.asarray(lengths, jnp.int32))

    lengths = jnp.where(number % 4 == 0, named(packed, number // 4), named(ordinary, number - number // 4 - 1))
    mixed = jax.random.permutation(jax.random.fold_in(own, 3), count)
    donor, taker = mixed[0:count // 2 * 2:2], mixed[1:count // 2 * 2:2]
    slack = jnp.minimum(lengths[donor] - 1, reach - lengths[taker]) // 2
    slack = jnp.where((donor == sequence[0]) | (taker == sequence[0]) | (lengths[taker] == 0), 0, jnp.maximum(slack, 0))
    moved = jax.random.randint(jax.random.fold_in(own, 4), (count // 2,), 0, 1 << 20) % (slack + 1)
    lengths = lengths.at[donor].add(-moved).at[taker].add(moved)
    items = jnp.searchsorted(jnp.cumsum(lengths), jnp.arange(rows * top), side="right").astype(jnp.int32)
    listing = items.reshape(top, rows).T
    listing = listing[jax.random.permutation(jax.random.fold_in(own, 1), rows)]
    turn = jax.random.randint(jax.random.fold_in(own, 2), (rows, 1), 0, top)
    return jnp.take_along_axis(listing, (jnp.arange(top)[None, :] + turn) % top, axis=1)


def shares(count, total, bound, slope, full):
    portions = [(1 << 20) // math.isqrt(rank ** slope) + 1 for rank in range(1, count + 1)]
    largest = bound if full else min(bound, max(-(-total // count), total * portions[0] // sum(portions)))
    least = 1 if total - largest >= count - 1 else 0
    holding, rest = [largest] + [least] * (count - 1), total - largest - least * (count - 1)
    while rest > 0:
        candidates = [i for i in range(1, count) if holding[i] < largest] or [i for i in range(1, count) if holding[i] < bound]
        mass, budget = sum([portions[i] for i in candidates]), rest
        for i in candidates:
            addition = min(bound - holding[i], max(1, budget * portions[i] // mass), rest)
            holding[i] = holding[i] + addition
            rest = rest - addition
    return np.array(holding)


def gaussian(stream_key, dims, width, limit, shards=(), kind=jnp.bfloat16):
    array = jax.random.normal(stream_key, dims, jnp.float32) * width
    if len(shards) > 0:
        array = shard_levels(stream_key, dims, shards, -0.22, 0.18) * array
    return jnp.clip(array, min=-limit, max=limit).astype(kind)


def setup_inputs(seed: int = 0) -> dict:
    arg_keys = jax.random.split(jax.random.key(seed), 8)
    x_in = gaussian(arg_keys[0], (MICRO, ROWS, D), 1.0, 6.0, ((1, 16), (2, 8)))
    cotangent = gaussian(arg_keys[1], (MICRO, ROWS, D), 1.0, 6.0, ((1, 16), (2, 8)))
    route_ids_keys = jax.random.split(jax.random.fold_in(arg_keys[2], 1), SECTIONS * MICRO * ROWS // TOK_DEV)
    route_ids_turns = jax.random.permutation(jax.random.fold_in(arg_keys[2], 3), SECTIONS * MICRO * ROWS // TOK_DEV)
    route_ids = jax.vmap(lambda own, number: routed_block(jax.random.fold_in(arg_keys[2], 2), own, number, TOK_DEV, EXPERTS, TOP, CAP, 2))(route_ids_keys, route_ids_turns).reshape((SECTIONS, MICRO, ROWS, TOP))
    norm_gain = jnp.clip(1.0 + 0.1 * jax.random.normal(arg_keys[3], (SECTIONS, D), jnp.float32), 0.5, 1.5)
    router = gaussian(arg_keys[4], (SECTIONS, D, EXPERTS), D ** -0.5, 0.125, ((0, 8),))
    w_gate_up = gaussian(arg_keys[5], (SECTIONS, EXPERTS, D, 2 * FFW), D ** -0.5, 0.125, ((0, 8), (1, 16)))
    w_down = gaussian(arg_keys[6], (SECTIONS, EXPERTS, FFW, D), FFW ** -0.5, 0.25, ((0, 8), (1, 16)))
    return dict(x_in=x_in, cotangent=cotangent, route_ids=route_ids, norm_gain=norm_gain, router=router, w_gate_up=w_gate_up, w_down=w_down)


EPS = 1e-05

def rounded(value):
    return lax.optimization_barrier(value.astype(jnp.bfloat16))

def slot_tables(route_rows):
    experts = jnp.arange(EXPERTS, dtype=jnp.int32)
    expert_hits = (route_rows[..., None] == experts).astype(jnp.int32)
    per_expert = lax.optimization_barrier(jnp.sum(expert_hits, axis=-2))
    before = jnp.cumsum(per_expert, axis=-2) - per_expert
    slot_ids = lax.optimization_barrier(jnp.sum(expert_hits * before[..., None, :], axis=-1))
    dest_cell = route_rows * CAP + slot_ids
    cell_ids = jnp.arange(EXPERTS * CAP, dtype=jnp.int32)
    slot_place = (dest_cell[..., None] == cell_ids).astype(jnp.float32)
    return (expert_hits.astype(jnp.float32), slot_place)

def layer_state(layer_in, route_rows, gain_vec, router_mat, w_gu):
    blocks = ROWS // TOK_DEV
    h_wide = layer_in.reshape(MICRO, blocks, TOK_DEV, D).astype(jnp.float32)
    inv_rms = lax.rsqrt(lax.optimization_barrier(jnp.mean(h_wide * h_wide, axis=-1, keepdims=True)) + EPS)
    normed = rounded(h_wide * inv_rms * gain_vec).astype(jnp.float32)
    expert_hits, slot_place = slot_tables(route_rows.reshape(MICRO, blocks, TOK_DEV, TOP))
    logits = jnp.einsum('mbtd,de->mbte', normed, router_mat.astype(jnp.float32), precision=lax.Precision.HIGHEST)
    chosen = lax.optimization_barrier(jnp.sum(expert_hits * logits[..., None, :], axis=-1))
    first_gate = jax.nn.sigmoid(chosen[..., 0] - chosen[..., 1])
    second_gate = jax.nn.sigmoid(chosen[..., 1] - chosen[..., 0])
    exp_rows = rounded(jnp.einsum('mbtkc,mbtd->mbcd', slot_place, normed, precision=lax.Precision.HIGHEST))
    exp_rows = exp_rows.astype(jnp.float32).reshape(MICRO, blocks, EXPERTS, CAP, D)
    gate_up = jnp.einsum('mbecd,edf->mbecf', exp_rows, w_gu.astype(jnp.float32), precision=lax.Precision.HIGHEST)
    gate_part = gate_up[..., :FFW]
    up_part = gate_up[..., FFW:]
    sigmoid_gate = jax.nn.sigmoid(gate_part)
    hidden = rounded(gate_part * sigmoid_gate * up_part).astype(jnp.float32)
    return (h_wide, inv_rms, normed, expert_hits, slot_place, first_gate, second_gate, exp_rows, gate_part, up_part, sigmoid_gate, hidden)

def expert_out(hidden, w_dn):
    blocks = ROWS // TOK_DEV
    out_rows = rounded(jnp.einsum('mbecf,efd->mbecd', hidden, w_dn.astype(jnp.float32), precision=lax.Precision.HIGHEST))
    return out_rows.astype(jnp.float32).reshape(MICRO, blocks, EXPERTS * CAP, D)

def forward_layer(layer_in, route_rows, gain_vec, router_mat, w_gu, w_dn):
    state = layer_state(layer_in, route_rows, gain_vec, router_mat, w_gu)
    h_wide, slot_place, first_gate, second_gate, hidden = (state[0], state[4], state[5], state[6], state[11])
    picked = jnp.einsum('mbtkc,mbcd->mbtkd', slot_place, expert_out(hidden, w_dn), precision=lax.Precision.HIGHEST)
    layer_out = h_wide + first_gate[..., None] * picked[..., 0, :] + second_gate[..., None] * picked[..., 1, :]
    return layer_out.astype(jnp.bfloat16).reshape(MICRO, ROWS, D)

def backward_layer(layer_in, grad_top, route_rows, gain_vec, router_mat, w_gu, w_dn):
    blocks = ROWS // TOK_DEV
    h_wide, inv_rms, normed, expert_hits, slot_place, first_gate, second_gate, exp_rows, gate_part, up_part, sigmoid_gate, hidden = layer_state(layer_in, route_rows, gain_vec, router_mat, w_gu)
    grad_wide = grad_top.reshape(MICRO, blocks, TOK_DEV, D).astype(jnp.float32)
    gates = jnp.stack([first_gate, second_gate], axis=-1)
    scaled = rounded(gates[..., None] * grad_wide[..., None, :]).astype(jnp.float32)
    dy_rows = rounded(jnp.einsum('mbtkc,mbtkd->mbcd', slot_place, scaled, precision=lax.Precision.HIGHEST))
    dy_rows = dy_rows.astype(jnp.float32).reshape(MICRO, blocks, EXPERTS, CAP, D)
    d_hidden = jnp.einsum('mbecd,efd->mbecf', dy_rows, w_dn.astype(jnp.float32), precision=lax.Precision.HIGHEST)
    silu_gate = gate_part * sigmoid_gate
    silu_slope = sigmoid_gate * (1.0 + gate_part * (1.0 - sigmoid_gate))
    gate_up_grad = rounded(jnp.concatenate([d_hidden * up_part * silu_slope, d_hidden * silu_gate], axis=-1))
    gate_up_grad = gate_up_grad.astype(jnp.float32)
    rows_grad = rounded(jnp.einsum('mbecf,edf->mbecd', gate_up_grad, w_gu.astype(jnp.float32), precision=lax.Precision.HIGHEST))
    rows_grad = rows_grad.astype(jnp.float32).reshape(MICRO, blocks, EXPERTS * CAP, D)
    grad_gu = jnp.einsum('mbecd,mbecf->edf', exp_rows, gate_up_grad, precision=lax.Precision.HIGHEST)
    grad_dn = jnp.einsum('mbecf,mbecd->efd', hidden, dy_rows, precision=lax.Precision.HIGHEST)
    normed_grad = jnp.einsum('mbtkc,mbcd->mbtd', slot_place, rows_grad, precision=lax.Precision.HIGHEST)
    picked = jnp.einsum('mbtkc,mbcd->mbtkd', slot_place, expert_out(hidden, w_dn), precision=lax.Precision.HIGHEST)
    gate_grad = lax.optimization_barrier(jnp.sum(grad_wide[..., None, :] * picked, axis=-1))
    logit_grad = first_gate * second_gate * (gate_grad[..., 0] - gate_grad[..., 1])
    logit_cols = logit_grad[..., None] * (expert_hits[..., 0, :] - expert_hits[..., 1, :])
    normed_grad = normed_grad + jnp.einsum('mbte,de->mbtd', logit_cols, router_mat.astype(jnp.float32), precision=lax.Precision.HIGHEST)
    grad_rt = jnp.einsum('mbtd,mbte->de', normed, logit_cols, precision=lax.Precision.HIGHEST)
    grad_gn = lax.optimization_barrier(jnp.sum(normed_grad * h_wide * inv_rms, axis=(0, 1, 2)))
    scaled_grad = normed_grad * gain_vec
    projection = lax.optimization_barrier(jnp.mean(scaled_grad * h_wide, axis=-1, keepdims=True))
    input_grad = grad_wide + inv_rms * scaled_grad - h_wide * inv_rms * inv_rms * inv_rms * projection
    return (input_grad.astype(jnp.bfloat16).reshape(MICRO, ROWS, D), (grad_gu, grad_dn, grad_rt, grad_gn))

def reference(x_in, cotangent, route_ids, norm_gain, router, w_gate_up, w_down):

    def forward_step(layer_in, params):
        route_rows, gain_vec, router_mat, w_gu, w_dn = params
        return (forward_layer(layer_in, route_rows, gain_vec, router_mat, w_gu, w_dn), layer_in)
    _, inputs = lax.scan(forward_step, x_in, (route_ids, norm_gain, router, w_gate_up, w_down))

    def backward_step(grad_top, params):
        route_rows, gain_vec, router_mat, w_gu, w_dn, layer_in = params
        return backward_layer(layer_in, grad_top, route_rows, gain_vec, router_mat, w_gu, w_dn)
    grad_in, grad_list = lax.scan(backward_step, cotangent, (route_ids, norm_gain, router, w_gate_up, w_down, inputs), reverse=True)
    return (grad_in, grad_list[0], grad_list[1], grad_list[2], grad_list[3])
```

```python
import functools

import jax
import jax.numpy as jnp
from jax import lax
from jax.experimental import pallas as pl
from jax.experimental.pallas import tpu as pltpu
from jax.sharding import PartitionSpec as P

EPS = 1e-05
GROUP = 1
LAG_E = 1
LAG_R = 3
BACK_E = 1
BACK_R = 3
LANES = 128
MESH = pl.DeviceIdType.MESH
F32 = jnp.float32
BF16 = jnp.bfloat16


def dot(lhs, rhs):
    return jnp.dot(lhs, rhs, preferred_element_type=F32)


def dot_nt(lhs, rhs):
    return lax.dot_general(lhs, rhs, (((1,), (1,)), ((), ())), preferred_element_type=F32)


def dot_tn(lhs, rhs):
    return lax.dot_general(lhs, rhs, (((0,), (0,)), ((), ())), preferred_element_type=F32)


def stack_kernel(
    sizes,
    x_ref, cot_ref, sel_ref, selt_ref, sign_ref, gain_ref, router_ref, wgu_ref, wdn_ref,
    rows_ref, q_ref, hid_ref, dyr_ref, gin_ref, red_ref,
    h_buf, g_buf, u_buf, hs_buf, gs_buf,
    xs_buf, xr_buf, ys_buf, yr_buf, ds_buf, dr_buf, us_buf, ur_buf,
    pick_buf, gate_buf, slope_buf, silu_buf, dul_buf, wide,
    acc_r, acc_g, red_s, red_r, gin_r,
    send_sem, recv_sem, line_send, line_recv, gather_send, gather_recv, gin_send, gin_recv, red_send, red_recv,
):
    ns, ny, nz, cap = sizes
    ne = ny * nz
    micro, tok, width = h_buf.shape
    part = width // ns
    cells = ne * cap
    blk = cap * (width // (2 * LANES))
    folds = width // (2 * LANES)
    group = GROUP
    chunks = micro // group
    ffw = wdn_ref.shape[0]
    sec = lax.axis_index("section")
    ey = lax.axis_index("expert")
    ez = lax.axis_index("dp")

    def ahead(k):
        return {"expert": lax.rem(ey + k // nz, ny), "dp": lax.rem(ez + k % nz, nz)}

    def behind(k):
        return {"expert": lax.rem(ey + ny - k // nz, ny), "dp": lax.rem(ez + nz - k % nz, nz)}

    def far(k):
        ky, kz = k // nz, k % nz
        return min(ky, ny - ky) + min(kz, nz - kz)

    order = sorted(range(1, ne), key=lambda k: -far(k))

    barrier = pltpu.get_barrier_semaphore()
    for k in range(1, ne):
        pl.semaphore_signal(barrier, inc=1, device_id=ahead(k), device_id_type=MESH)
    for step in range(1, ns):
        pl.semaphore_signal(
            barrier, inc=1, device_id={"section": lax.rem(sec + step, ns)}, device_id_type=MESH
        )
    pl.semaphore_wait(barrier, ne - 1 + ns - 1)

    my_cols = pl.ds(pl.multiple_of(sec * part, LANES), part)

    def gather_copy(which, src, dst, owner):
        return pltpu.make_async_remote_copy(
            src_ref=src, dst_ref=dst.at[:, :, my_cols],
            send_sem=gather_send.at[which], recv_sem=gather_recv.at[which],
            device_id={"section": owner}, device_id_type=MESH,
        )

    @pl.when(sec != 0)
    def _():
        gather_copy(0, x_ref, h_buf, 0).start()

    @pl.when(sec != ns - 1)
    def _():
        gather_copy(1, cot_ref, g_buf, ns - 1).start()

    @pl.when(sec == 0)
    def _():
        h_buf[:, :, 0:part] = x_ref[...]

    @pl.when(sec == ns - 1)
    def _():
        g_buf[:, :, (ns - 1) * part :] = cot_ref[...]

    acc_r[...] = jnp.zeros_like(acc_r)
    acc_g[...] = jnp.zeros_like(acc_g)

    def span(chunk):
        return pl.ds(chunk * group, group)

    def exchange(kind, chunk, src, dst, target):
        for k in order:
            rows = pl.ds(k * blk, blk)
            pltpu.make_async_remote_copy(
                src_ref=src.at[span(chunk), rows], dst_ref=dst.at[span(chunk), rows],
                send_sem=send_sem.at[kind, chunk], recv_sem=recv_sem.at[kind, chunk],
                device_id=target(k), device_id_type=MESH,
            ).start()

    def arrived(kind, chunk, dst):
        part_ref = dst.at[span(chunk), pl.ds(blk, (ne - 1) * blk)]
        pltpu.make_async_copy(part_ref, part_ref, recv_sem.at[kind, chunk]).wait()

    def fold(value, at, send, recv):
        for j in range(folds):
            for half in range(2):
                left = (2 * j + half) * LANES
                wide[half, pl.ds(j, cells, stride=folds), :] = value[:, left : left + LANES]
        for half in range(2):
            cols = slice(half * LANES, (half + 1) * LANES)
            packed = wide[half].astype(BF16)
            send[at, :, cols] = packed
            recv[at, 0:blk, cols] = packed[0:blk]

    def unfold(at, recv):
        for half in range(2):
            wide[half] = recv[at, :, half * LANES : (half + 1) * LANES].astype(F32)
        pieces = [
            wide[half, pl.ds(j, cells, stride=folds), :] for j in range(folds) for half in range(2)
        ]
        return jnp.concatenate(pieces, axis=1).astype(BF16)

    def line_copy(way, chunk, src, dst, target):
        return pltpu.make_async_remote_copy(
            src_ref=src.at[span(chunk)], dst_ref=dst.at[span(chunk)],
            send_sem=line_send.at[way, chunk], recv_sem=line_recv.at[way, chunk],
            device_id={"section": target}, device_id_type=MESH,
        )

    def inv_rms(h_wide):
        return lax.rsqrt(jnp.mean(h_wide * h_wide, axis=-1, keepdims=True) + EPS)

    def wait_gather(which, dst):
        part_ref = dst.at[:, :, pl.ds(0, (ns - 1) * part)]
        pltpu.make_async_copy(part_ref, part_ref, gather_recv.at[which]).wait()

    def tokens_out(chunk):
        @pl.when((sec == 0) & (chunk == 0))
        def _():
            wait_gather(0, h_buf)

        @pl.when(sec != 0)
        def _():
            line_copy(0, chunk, hs_buf, h_buf, 0).wait_recv()

        for n in range(group):
            at = chunk * group + n
            h_wide = h_buf[at].astype(F32)
            normed = (h_wide * inv_rms(h_wide) * gain_ref[...]).astype(BF16)
            u_buf[at] = normed
            both = jnp.concatenate([normed, normed], axis=0)
            fold(dot(selt_ref[at], both), at, xs_buf, xr_buf)
        exchange(0, chunk, xs_buf, xr_buf, ahead)
        for n in range(group):
            at = chunk * group + n
            logits = dot_nt(u_buf[at], router_ref[...])
            gap = jnp.sum(logits * sign_ref[at], axis=-1, keepdims=True)
            gates = jnp.concatenate([jax.nn.sigmoid(gap), jax.nn.sigmoid(-gap)], axis=0)
            gate_buf[at] = jnp.broadcast_to(gates, (2 * tok, LANES))

    def experts(chunk):
        arrived(0, chunk, xr_buf)
        rows = pl.ds(pl.multiple_of(chunk * group * cells, cells), group * cells)
        for n in range(group):
            at = chunk * group + n
            rows_ref[pl.ds(pl.multiple_of(at * cells, cells), cells), :] = unfold(at, xr_buf)
        gate_up = dot(rows_ref[rows, :], wgu_ref[...])
        gate_part = gate_up[:, :ffw]
        up_part = gate_up[:, ffw:]
        sig = jax.nn.sigmoid(gate_part)
        silu = gate_part * sig
        hidden = (silu * up_part).astype(BF16)
        hid_ref[rows, :] = hidden
        out = dot(hidden, wdn_ref[...])
        for n in range(group):
            fold(out[n * cells : (n + 1) * cells], chunk * group + n, ys_buf, yr_buf)
        exchange(1, chunk, ys_buf, yr_buf, behind)
        silu_buf[rows, :] = silu
        slope_buf[rows, :] = up_part * (sig * (1.0 + gate_part * (1.0 - sig)))

    def tokens_in(chunk):
        arrived(1, chunk, yr_buf)
        for n in range(group):
            at = chunk * group + n
            picked = dot(sel_ref[at], unfold(at, yr_buf))
            pick_buf[at] = picked.astype(BF16)
            gates = gate_buf[at][:, :1]
            total = h_buf[at].astype(F32) + gates[:tok] * picked[:tok] + gates[tok:] * picked[tok:]
            hs_buf[at] = total.astype(BF16)

        @pl.when(sec != ns - 1)
        def _():
            line_copy(0, chunk, hs_buf, h_buf, sec + 1).start()

    def schedule(first, second, third, lag_second, lag_third):
        def step(i, carry):
            @pl.when(i < chunks)
            def _():
                first(i)

            @pl.when((i >= lag_second) & (i < chunks + lag_second))
            def _():
                second(i - lag_second)

            @pl.when(i >= lag_third)
            def _():
                third(i - lag_third)

            return carry

        lax.fori_loop(0, chunks + lag_third, step, 0)

    schedule(tokens_out, experts, tokens_in, LAG_E, LAG_R)

    def grads_out(chunk):
        @pl.when((sec == ns - 1) & (chunk == 0))
        def _():
            wait_gather(1, g_buf)

        @pl.when(sec != ns - 1)
        def _():
            line_copy(1, chunk, gs_buf, g_buf, 0).wait_recv()

        for n in range(group):
            at = chunk * group + n
            grad = g_buf[at].astype(F32)
            gates = gate_buf[at][:, :1]
            scaled = (jnp.concatenate([grad, grad], axis=0) * gates).astype(BF16)
            fold(dot(selt_ref[at], scaled), at, ds_buf, dr_buf)
        exchange(2, chunk, ds_buf, dr_buf, ahead)
        for n in range(group):
            at = chunk * group + n
            grad = g_buf[at].astype(F32)
            gates = gate_buf[at][:, :1]
            picked = pick_buf[at].astype(F32)
            diff = jnp.sum(grad * (picked[:tok] - picked[tok:]), axis=-1, keepdims=True)
            cols = (gates[:tok] * gates[tok:] * diff * sign_ref[at]).astype(BF16)
            dul_buf[at] = dot(cols, router_ref[...])
            acc_r[...] += dot_tn(cols, u_buf[at])

    def expert_grads(chunk):
        arrived(2, chunk, dr_buf)
        rows = pl.ds(pl.multiple_of(chunk * group * cells, cells), group * cells)
        for n in range(group):
            at = chunk * group + n
            dyr_ref[pl.ds(pl.multiple_of(at * cells, cells), cells), :] = unfold(at, dr_buf)
        d_hidden = dot_nt(dyr_ref[rows, :], wdn_ref[...])
        q_ref[rows, :ffw] = (d_hidden * slope_buf[rows, :]).astype(BF16)
        q_ref[rows, ffw:] = (d_hidden * silu_buf[rows, :]).astype(BF16)
        out = dot_nt(q_ref[rows, :], wgu_ref[...])
        for n in range(group):
            fold(out[n * cells : (n + 1) * cells], chunk * group + n, us_buf, ur_buf)
        exchange(3, chunk, us_buf, ur_buf, behind)

    def gin_copy(chunk, target):
        return pltpu.make_async_remote_copy(
            src_ref=gs_buf.at[span(chunk), :, pl.ds(target * part, part)],
            dst_ref=gin_r.at[span(chunk)],
            send_sem=gin_send.at[target, chunk], recv_sem=gin_recv.at[chunk],
            device_id={"section": target}, device_id_type=MESH,
        )

    def grads_in(chunk):
        arrived(3, chunk, ur_buf)
        for n in range(group):
            at = chunk * group + n
            picked = dot(sel_ref[at], unfold(at, ur_buf))
            grad_u = picked[:tok] + picked[tok:] + dul_buf[at]
            h_wide = h_buf[at].astype(F32)
            inv = inv_rms(h_wide)
            scaled = grad_u * gain_ref[...]
            proj = jnp.mean(scaled * h_wide, axis=-1, keepdims=True)
            grad = g_buf[at].astype(F32) + inv * scaled - h_wide * (inv * inv * inv * proj)
            gs_buf[at] = grad.astype(BF16)

        @pl.when(sec != 0)
        def _():
            line_copy(1, chunk, gs_buf, g_buf, sec - 1).start()

        @pl.when(sec == 0)
        def _():
            for target in range(1, ns):
                gin_copy(chunk, target).start()
            gin_ref[span(chunk)] = gs_buf[span(chunk), :, 0:part]

        for n in range(group):
            at = chunk * group + n
            picked = dot(sel_ref[at], unfold(at, ur_buf))
            grad_u = picked[:tok] + picked[tok:] + dul_buf[at]
            h_wide = h_buf[at].astype(F32)
            acc_g[...] += jnp.sum(grad_u * h_wide * inv_rms(h_wide), axis=0, keepdims=True)

    schedule(grads_out, expert_grads, grads_in, BACK_E, BACK_R)

    red_s[:, :width] = acc_r[...].astype(BF16)
    per = width // ne
    gains = [acc_g[:, i * per : (i + 1) * per] for i in range(ne)]
    red_s[:, width:] = jnp.concatenate(gains, axis=0).astype(BF16)

    def red_copy(k):
        return pltpu.make_async_remote_copy(
            src_ref=red_s, dst_ref=red_r.at[k],
            send_sem=red_send, recv_sem=red_recv,
            device_id=ahead(k), device_id_type=MESH,
        )

    for k in order:
        red_copy(k).start()

    @pl.when(sec != 0)
    def _():
        def take(chunk, carry):
            dst = gin_r.at[span(chunk)]
            pltpu.make_async_copy(dst, dst, gin_recv.at[chunk]).wait()
            return carry

        lax.fori_loop(0, chunks, take, 0)
        gin_ref[...] = gin_r[...]

    others = red_r.at[pl.ds(1, ne - 1)]
    pltpu.make_async_copy(others, others, red_recv).wait()
    total = red_s[...].astype(F32)
    for k in range(1, ne):
        total = total + red_r[k].astype(F32)
    red_ref[...] = total

    pltpu.make_async_copy(others, others, red_send).wait()

    def drain(chunk, carry):
        for kind, buf in enumerate((xs_buf, ys_buf, ds_buf, us_buf)):
            part_ref = buf.at[span(chunk), pl.ds(blk, (ne - 1) * blk)]
            pltpu.make_async_copy(part_ref, part_ref, send_sem.at[kind, chunk]).wait()

        @pl.when(sec != ns - 1)
        def _():
            line_copy(0, chunk, hs_buf, h_buf, 0).wait_send()

        @pl.when(sec != 0)
        def _():
            line_copy(1, chunk, gs_buf, g_buf, 0).wait_send()

        @pl.when(sec == 0)
        def _():
            for target in range(1, ns):
                gin_copy(chunk, target).wait_send()

        return carry

    lax.fori_loop(0, chunks, drain, 0)

    @pl.when(sec != 0)
    def _():
        gather_copy(0, x_ref, h_buf, 0).wait_send()

    @pl.when(sec != ns - 1)
    def _():
        gather_copy(1, cot_ref, g_buf, ns - 1).wait_send()


def slot_tables(route_rows, n_expert, capacity, ny, nz):
    micro, tok, _ = route_rows.shape
    ey, ez = lax.axis_index("expert"), lax.axis_index("dp")
    named = jnp.transpose(route_rows, (0, 2, 1)).reshape(micro, 2 * tok)
    token = jnp.arange(2 * tok, dtype=jnp.int32) % tok
    same = (named[:, :, None] == named[:, None, :]) & (token[None, :] < token[:, None])
    slot = jnp.sum(same.astype(jnp.int32), axis=2)
    rel = ((named // nz - ey) % ny) * nz + (named % nz - ez) % nz
    cell = rel * capacity + slot
    ids = jnp.arange(n_expert * capacity, dtype=jnp.int32)
    sel = (cell[:, :, None] == ids).astype(BF16)
    selt = (cell[:, None, :] == ids[:, None]).astype(BF16)
    experts = jnp.arange(n_expert, dtype=jnp.int32)
    hits = (named[:, :, None] == experts).astype(F32)
    sign = hits[:, :tok] - hits[:, tok:]
    return sel, selt, sign


def local(x_in, cotangent, route_ids, norm_gain, router, w_gate_up, w_down):
    ns, ny, nz = (lax.axis_size(a) for a in ("section", "expert", "dp"))
    micro, tok, part = x_in.shape
    width = part * ns
    ne = ny * nz
    cap = 2 * tok // ne
    cells = ne * cap
    ffw = w_down.shape[2]
    chunks = micro // GROUP
    sel, selt, sign = slot_tables(route_ids[0], ne, cap, ny, nz)
    wire = pltpu.VMEM((micro, cells * width // (2 * LANES), 2 * LANES), BF16)
    rows = pltpu.VMEM((micro, tok, width), BF16)
    dma = pltpu.SemaphoreType.DMA
    red_width = width + width // ne
    scratch = (
        [rows] * 5
        + [wire] * 8
        + [
            pltpu.VMEM((micro, 2 * tok, width), BF16),
            pltpu.VMEM((micro, 2 * tok, LANES), F32),
            pltpu.VMEM((micro * cells, ffw), F32),
            pltpu.VMEM((micro * cells, ffw), F32),
            pltpu.VMEM((micro, tok, width), F32),
            pltpu.VMEM((2, cells * width // (2 * LANES), LANES), F32),
            pltpu.VMEM((ne, width), F32),
            pltpu.VMEM((1, width), F32),
            pltpu.VMEM((ne, red_width), BF16),
            pltpu.VMEM((ne, ne, red_width), BF16),
            pltpu.VMEM((micro, tok, part), BF16),
            dma((4, chunks)), dma((4, chunks)), dma((2, chunks)), dma((2, chunks)),
            dma((2,)), dma((2,)), dma((ns, chunks)), dma((chunks,)), dma, dma,
        ]
    )
    outs = (
        jax.ShapeDtypeStruct((micro * cells, width), BF16),
        jax.ShapeDtypeStruct((micro * cells, 2 * ffw), BF16),
        jax.ShapeDtypeStruct((micro * cells, ffw), BF16),
        jax.ShapeDtypeStruct((micro * cells, width), BF16),
        jax.ShapeDtypeStruct((micro, tok, part), BF16),
        jax.ShapeDtypeStruct((ne, red_width), F32),
    )
    exp_rows, q, hidden, dy_rows, grad_in, red = pl.pallas_call(
        functools.partial(stack_kernel, (ns, ny, nz, cap)),
        out_shape=outs,
        in_specs=[pl.BlockSpec(memory_space=pltpu.VMEM)] * 9,
        out_specs=[pl.BlockSpec(memory_space=pltpu.VMEM)] * 6,
        scratch_shapes=scratch,
        compiler_params=pltpu.CompilerParams(
            collective_id=0, has_side_effects=True, vmem_limit_bytes=60 * 1024 * 1024
        ),
    )(
        x_in, cotangent, sel, selt, sign, norm_gain, router[0].T,
        w_gate_up[0, 0], w_down[0, 0],
    )
    grad_gu = dot_tn(exp_rows, q)
    grad_dn = dot_tn(hidden, dy_rows)
    sum_router = red[:, :width].T
    sum_gain = red[:, width:].reshape(width)
    return grad_in, grad_gu[None, None], grad_dn[None, None], sum_router[None], sum_gain[None]


def solution(mesh):
    in_specs = (
        P(None, ("expert", "dp"), "section"),
        P(None, ("expert", "dp"), "section"),
        P("section", None, ("expert", "dp"), None),
        P("section", None),
        P("section", None, None),
        P("section", ("expert", "dp"), None, None),
        P("section", ("expert", "dp"), None, None),
    )
    out_specs = (
        P(None, ("expert", "dp"), "section"),
        P("section", ("expert", "dp"), None, None),
        P("section", ("expert", "dp"), None, None),
        P("section", None, None),
        P("section", None),
    )
    return jax.shard_map(local, mesh=mesh, in_specs=in_specs, out_specs=out_specs, check_vma=False)
```

```python
import functools

import jax
import jax.numpy as jnp
from jax import lax
from jax.experimental import pallas as pl
from jax.experimental.pallas import tpu as pltpu
from jax.sharding import PartitionSpec as P

EPS = 1e-05
GROUP = 1
LAG = 1
BETWEEN = 5
LANES = 128
MESH = pl.DeviceIdType.MESH
F32 = jnp.float32
BF16 = jnp.bfloat16


def dot(lhs, rhs):
    return jnp.dot(lhs, rhs, preferred_element_type=F32)


def dot_nt(lhs, rhs):
    return lax.dot_general(lhs, rhs, (((1,), (1,)), ((), ())), preferred_element_type=F32)


def dot_tn(lhs, rhs):
    return lax.dot_general(lhs, rhs, (((0,), (0,)), ((), ())), preferred_element_type=F32)


def stack_kernel(
    sizes,
    x_ref, cot_ref, route_ref, gain_ref, router_ref, wgu_hbm, wdn_hbm,
    rows_hbm, q_hbm, hid_hbm, dyr_hbm, gin_ref, router_sum_ref, gain_sum_ref,
    wgu_ref, wdn_ref, rows_ref, q_ref, hid_ref, dyr_ref, tab, tab_in, sign_ref,
    h_buf, hin_buf, g_buf, u_buf, gs_buf,
    xs_buf, xr_buf, ys_buf, yr_buf, yl_buf, ds_buf, dn_buf, dr_buf, us_buf, ur_buf,
    pick_buf, gate_buf, gatein_buf, l_buf, ls_buf, slope_buf, silu_buf, dul_buf, wide,
    acc_r, acc_g, part_s, part_r, sum_s, sum_r, gain_s, gain_r, gin_r,
    send_sem, recv_sem, line_send, line_recv, tab_sem, gather_send, gather_recv, gin_send, gin_recv,
    red_send, red_recv, local_sem,
):
    ns, ny, nz, cap = sizes
    ne = ny * nz
    micro, tok, width = h_buf.shape
    part = width // ns
    cells = ne * cap
    blk = cap * (width // (2 * LANES))
    folds = width // (2 * LANES)
    group = GROUP
    chunks = micro // group
    ffw = wdn_ref.shape[0]
    sec = lax.axis_index("section")
    ey = lax.axis_index("expert")
    ez = lax.axis_index("dp")

    first, last = sec == 0, sec == ns - 1
    inner, lower = sec != ns - 1, sec != 0

    def ahead(k, section=None):
        there = {"expert": lax.rem(ey + k // nz, ny), "dp": lax.rem(ez + k % nz, nz)}
        return there if section is None else {"section": section, **there}

    def behind(k, section=None):
        there = {"expert": lax.rem(ey + ny - k // nz, ny), "dp": lax.rem(ez + nz - k % nz, nz)}
        return there if section is None else {"section": section, **there}

    def far(k):
        ky, kz = k // nz, k % nz
        return min(ky, ny - ky) + min(kz, nz - kz)

    order = sorted(range(1, ne), key=lambda k: -far(k))
    order_all = order + [0]

    loads = [
        pltpu.make_async_copy(src, dst, local_sem.at[n])
        for n, (src, dst) in enumerate(((wgu_hbm, wgu_ref), (wdn_hbm, wdn_ref)))
    ]
    stores = [
        pltpu.make_async_copy(src, dst, local_sem.at[2 + n])
        for n, (src, dst) in enumerate(
            ((rows_ref, rows_hbm), (hid_ref, hid_hbm), (dyr_ref, dyr_hbm), (q_ref, q_hbm))
        )
    ]
    for load in loads:
        load.start()

    barrier = pltpu.get_barrier_semaphore()
    for k in range(1, ne):
        pl.semaphore_signal(barrier, inc=1, device_id=ahead(k), device_id_type=MESH)
        for step in (1, ns - 1):
            there = ahead(k, lax.rem(sec + step, ns))
            pl.semaphore_signal(barrier, inc=1, device_id=there, device_id_type=MESH)
    for step in range(1, ns):
        pl.semaphore_signal(
            barrier, inc=1, device_id={"section": lax.rem(sec + step, ns)}, device_id_type=MESH
        )
    pl.semaphore_wait(barrier, 3 * (ne - 1) + ns - 1)

    my_cols = pl.ds(pl.multiple_of(sec * part, LANES), part)

    def gather_copy(which, src, dst, first, count, owner):
        at = pl.ds(first, count)
        return pltpu.make_async_remote_copy(
            src_ref=src.at[at], dst_ref=dst.at[at, :, my_cols],
            send_sem=gather_send.at[which], recv_sem=gather_recv.at[which],
            device_id={"section": owner}, device_id_type=MESH,
        )

    gathers = (
        gather_copy(0, x_ref, h_buf, 0, group, 0),
        gather_copy(1, x_ref, h_buf, group, micro - group, 0),
        gather_copy(2, cot_ref, g_buf, 0, micro, ns - 1),
    )

    @pl.when(sec != 0)
    def _():
        gathers[0].start()
        gathers[1].start()

    @pl.when(sec != ns - 1)
    def _():
        gathers[2].start()

    @pl.when(sec == 0)
    def _():
        h_buf[:, :, 0:part] = x_ref[...]

    @pl.when(sec == ns - 1)
    def _():
        g_buf[:, :, (ns - 1) * part :] = cot_ref[...]

    kinds = lax.broadcasted_iota(jnp.int32, (ne, tok), 0)
    place = jnp.zeros((ne, tok), F32)
    for e in range(ne):
        rel = lax.rem(e // nz + ny - ey, ny) * nz + lax.rem(e % nz + nz - ez, nz)
        place = jnp.where(kinds == e, (rel * cap).astype(F32), place)
    earlier = lax.broadcasted_iota(jnp.int32, (tok, tok), 0)
    earlier = (earlier < lax.broadcasted_iota(jnp.int32, (tok, tok), 1)).astype(BF16)
    cell_ids = lax.broadcasted_iota(jnp.int32, (cells, tok), 0).astype(F32)

    def eye(n):
        rows_id = lax.broadcasted_iota(jnp.int32, (n, n), 0)
        return (rows_id == lax.broadcasted_iota(jnp.int32, (n, n), 1)).astype(BF16)

    def tables(at, carry):
        named = route_ref[at]
        hits = [(kinds == named[k : k + 1, :]).astype(F32) for k in range(2)]
        before = dot((hits[0] + hits[1]).astype(BF16), earlier) + place
        for k in range(2):
            cell = jnp.sum(hits[k] * before, axis=0, keepdims=True)
            tab[at, 2 * tok :, k * tok : (k + 1) * tok] = (cell_ids == cell).astype(BF16)
        turned = dot_nt(eye(2 * tok), tab[at, 2 * tok :, : 2 * tok])
        tab[at, : 2 * tok, :cells] = turned.astype(BF16)
        sign_ref[at] = dot_nt(eye(tok), (hits[0] - hits[1]).astype(BF16))
        return carry

    tab[...] = jnp.zeros_like(tab)
    lax.fori_loop(0, micro, tables, 0)

    def table_copy(target):
        return pltpu.make_async_remote_copy(
            src_ref=tab, dst_ref=tab_in, send_sem=tab_sem.at[0], recv_sem=tab_sem.at[1],
            device_id={"section": target}, device_id_type=MESH,
        )

    @pl.when(inner)
    def _():
        table_copy(sec + 1).start()

    def pick(table, at):
        return table[at, : 2 * tok, :cells]

    def put(table, at):
        return table[at, 2 * tok :, : 2 * tok]

    acc_r[...] = jnp.zeros_like(acc_r)
    acc_g[...] = jnp.zeros_like(acc_g)

    def span(chunk):
        return pl.ds(chunk * group, group)

    def exchange(sent, kind, chunk, src, dst, target, blocks):
        for k in blocks:
            rows = pl.ds(k * blk, blk)
            pltpu.make_async_remote_copy(
                src_ref=src.at[span(chunk), rows], dst_ref=dst.at[span(chunk), rows],
                send_sem=send_sem.at[sent, chunk], recv_sem=recv_sem.at[kind, chunk],
                device_id=target(k), device_id_type=MESH,
            ).start()

    def wait_all(ref, sem):
        pltpu.make_async_copy(ref, ref, sem).wait()

    def others(buf, chunk):
        return buf.at[span(chunk), pl.ds(blk, (ne - 1) * blk)]

    def arrived(kind, chunk, dst):
        wait_all(others(dst, chunk), recv_sem.at[kind, chunk])

    def all_arrived(kind, chunk, dst):
        wait_all(dst.at[span(chunk)], recv_sem.at[kind, chunk])

    def fold(value, at, send, recv=None):
        for j in range(folds):
            for half in range(2):
                left = (2 * j + half) * LANES
                wide[half, pl.ds(j, cells, stride=folds), :] = value[:, left : left + LANES]
        for half in range(2):
            cols = slice(half * LANES, (half + 1) * LANES)
            packed = wide[half].astype(BF16)
            send[at, :, cols] = packed
            if recv is not None:
                recv[at, 0:blk, cols] = packed[0:blk]

    def unfold(at, recv):
        for half in range(2):
            wide[half] = recv[at, :, half * LANES : (half + 1) * LANES].astype(F32)
        pieces = [
            wide[half, pl.ds(j, cells, stride=folds), :] for j in range(folds) for half in range(2)
        ]
        return jnp.concatenate(pieces, axis=1).astype(BF16)

    def line_copy(way, chunk, src, dst, target):
        return pltpu.make_async_remote_copy(
            src_ref=src.at[span(chunk)], dst_ref=dst.at[span(chunk)],
            send_sem=line_send.at[way, chunk], recv_sem=line_recv.at[way, chunk],
            device_id={"section": target}, device_id_type=MESH,
        )

    def inv_rms(h_wide):
        return lax.rsqrt(jnp.mean(h_wide * h_wide, axis=-1, keepdims=True) + EPS)

    def wait_gather(which, dst, first, count):
        part_ref = dst.at[pl.ds(first, count), :, pl.ds(0, (ns - 1) * part)]
        pltpu.make_async_copy(part_ref, part_ref, gather_recv.at[which]).wait()

    line_h, line_gate, line_g, line_l = range(4)

    def up(way, chunk, target=0):
        pair = (h_buf, hin_buf) if way == line_h else (gate_buf, gatein_buf)
        return line_copy(way, chunk, *pair, target)

    def down(way, chunk, target=0):
        pair = (gs_buf, g_buf) if way == line_g else (ls_buf, l_buf)
        return line_copy(way, chunk, *pair, target)

    def tokens(chunk):
        @pl.when(first & (chunk == 0))
        def _():
            wait_gather(0, h_buf, 0, group)

        @pl.when(first & (chunk == 1))
        def _():
            wait_gather(1, h_buf, group, micro - group)

        @pl.when(lower & (chunk == 0))
        def _():
            table_copy(0).wait_recv()

        @pl.when(lower)
        def _():
            up(line_h, chunk).wait_recv()
            up(line_gate, chunk).wait_recv()
            all_arrived(1, chunk, yr_buf)
            for n in range(group):
                at = chunk * group + n
                picked = dot(pick(tab_in, at), unfold(at, yr_buf))
                gates = gatein_buf[at][:, :1]
                total = gates[:tok] * picked[:tok] + gates[tok:] * picked[tok:]
                h_buf[at] = (hin_buf[at].astype(F32) + total).astype(BF16)
                pick_buf[at] = picked.astype(BF16)

        for n in range(group):
            at = chunk * group + n
            h_wide = h_buf[at].astype(F32)
            normed = (h_wide * inv_rms(h_wide) * gain_ref[...]).astype(BF16)
            u_buf[at] = normed
            both = jnp.concatenate([normed, normed], axis=0)
            fold(dot(put(tab, at), both), at, xs_buf, xr_buf)
        exchange(0, 0, chunk, xs_buf, xr_buf, ahead, order)
        for n in range(group):
            at = chunk * group + n
            logits = dot_nt(u_buf[at], router_ref[...])
            gap = jnp.sum(logits * sign_ref[at], axis=-1, keepdims=True)
            gates = jnp.concatenate([jax.nn.sigmoid(gap), jax.nn.sigmoid(-gap)], axis=0)
            gate_buf[at] = jnp.broadcast_to(gates, (2 * tok, LANES))

        @pl.when(inner)
        def _():
            up(line_h, chunk, sec + 1).start()
            up(line_gate, chunk, sec + 1).start()

        @pl.when(last & (chunk == 0))
        def _():
            wait_gather(2, g_buf, 0, micro)

        @pl.when(last)
        def _():
            for n in range(group):
                at = chunk * group + n
                send_grad(at, g_buf[at].astype(F32), gate_buf, tab, ds_buf, dr_buf)
            exchange(2, 2, chunk, ds_buf, dr_buf, ahead, order)

    def send_grad(at, grad, gate_ref, table, send, recv=None):
        scaled = (jnp.concatenate([grad, grad], axis=0) * gate_ref[at][:, :1]).astype(BF16)
        fold(dot(put(table, at), scaled), at, send, recv)

    def experts(chunk):
        @pl.when(chunk == 0)
        def _():
            for load in loads:
                load.wait()

        arrived(0, chunk, xr_buf)
        rows = pl.ds(pl.multiple_of(chunk * group * cells, cells), group * cells)
        for n in range(group):
            at = chunk * group + n
            rows_ref[pl.ds(pl.multiple_of(at * cells, cells), cells), :] = unfold(at, xr_buf)
        gate_up = dot(rows_ref[rows, :], wgu_ref[...])
        gate_part = gate_up[:, :ffw]
        up_part = gate_up[:, ffw:]
        sig = jax.nn.sigmoid(gate_part)
        silu = gate_part * sig
        hidden = (silu * up_part).astype(BF16)
        hid_ref[rows, :] = hidden
        out = dot(hidden, wdn_ref[...])
        for n in range(group):
            fold(out[n * cells : (n + 1) * cells], chunk * group + n, ys_buf)

        @pl.when(inner)
        def _():
            exchange(1, 1, chunk, ys_buf, yr_buf, lambda k: behind(k, sec + 1), order_all)

        @pl.when(last)
        def _():
            exchange(1, 4, chunk, ys_buf, yl_buf, behind, order)
            yl_buf[span(chunk), 0:blk] = ys_buf[span(chunk), 0:blk]

        silu_buf[rows, :] = silu
        slope_buf[rows, :] = up_part * (sig * (1.0 + gate_part * (1.0 - sig)))

        @pl.when(chunk == chunks - 1)
        def _():
            stores[0].start()
            stores[1].start()

    piece = width // ne
    me = ey * nz + ez
    my_piece = pl.ds(pl.multiple_of(me * piece, LANES), piece)

    def part_copy(k):
        there = lax.rem(ey + k // nz, ny) * nz + lax.rem(ez + k % nz, nz)
        return pltpu.make_async_remote_copy(
            src_ref=part_s.at[:, pl.ds(pl.multiple_of(there * piece, LANES), piece)],
            dst_ref=part_r.at[k], send_sem=red_send.at[0], recv_sem=red_recv.at[0],
            device_id=ahead(k), device_id_type=MESH,
        )

    def sum_copy(k):
        return pltpu.make_async_remote_copy(
            src_ref=sum_s, dst_ref=sum_r.at[:, my_piece],
            send_sem=red_send.at[1], recv_sem=red_recv.at[1],
            device_id=ahead(k), device_id_type=MESH,
        )

    def gain_copy(k):
        return pltpu.make_async_remote_copy(
            src_ref=gain_s, dst_ref=gain_r.at[k],
            send_sem=red_send.at[2], recv_sem=red_recv.at[2],
            device_id=ahead(k), device_id_type=MESH,
        )

    def slope_of_gates(at, picked, gate_ref, out):
        gates = gate_ref[at][:, :1]
        grad = (g_buf if out is l_buf else gs_buf)[at].astype(F32)
        diff = jnp.sum(grad * (picked[:tok] - picked[tok:]), axis=-1, keepdims=True)
        out[at] = jnp.broadcast_to(gates[:tok] * gates[tok:] * diff, (tok, LANES))

    def route_grads(chunk):
        for n in range(group):
            at = chunk * group + n
            cols = (l_buf[at][:, :1] * sign_ref[at]).astype(BF16)
            dul_buf[at] = dot(cols, router_ref[...])
            acc_r[...] += dot_tn(cols, u_buf[at])

        @pl.when(chunk == chunks - 1)
        def _():
            part_s[...] = acc_r[...].astype(BF16)
            for k in order:
                part_copy(k).start()

    def sum_pieces():
        wait_all(part_r.at[pl.ds(1, ne - 1)], red_recv.at[0])
        total = part_s[:, my_piece].astype(F32)
        for k in range(1, ne):
            total = total + part_r[k].astype(F32)
        sum_s[...] = total
        sum_r[:, my_piece] = total
        for k in order:
            sum_copy(k).start()

    def expert_grads(chunk):
        @pl.when(inner)
        def _():
            all_arrived(2, chunk, dr_buf)

        @pl.when(last)
        def _():
            arrived(2, chunk, dr_buf)

        rows = pl.ds(pl.multiple_of(chunk * group * cells, cells), group * cells)
        for n in range(group):
            at = chunk * group + n
            dyr_ref[pl.ds(pl.multiple_of(at * cells, cells), cells), :] = unfold(at, dr_buf)
        d_hidden = dot_nt(dyr_ref[rows, :], wdn_ref[...])
        q_ref[rows, :ffw] = (d_hidden * slope_buf[rows, :]).astype(BF16)
        q_ref[rows, ffw:] = (d_hidden * silu_buf[rows, :]).astype(BF16)
        out = dot_nt(q_ref[rows, :], wgu_ref[...])
        for n in range(group):
            fold(out[n * cells : (n + 1) * cells], chunk * group + n, us_buf, ur_buf)
        exchange(3, 3, chunk, us_buf, ur_buf, behind, order)

        @pl.when(chunk == chunks - 1)
        def _():
            stores[2].start()
            stores[3].start()

        @pl.when(inner)
        def _():
            down(line_l, chunk).wait_recv()
            route_grads(chunk)

    def gin_copy(chunk, target):
        return pltpu.make_async_remote_copy(
            src_ref=gs_buf.at[span(chunk), :, pl.ds(target * part, part)],
            dst_ref=gin_r.at[span(chunk)],
            send_sem=gin_send.at[target, chunk], recv_sem=gin_recv.at[chunk],
            device_id={"section": target}, device_id_type=MESH,
        )

    def grads(chunk):
        @pl.when(last)
        def _():
            arrived(4, chunk, yl_buf)
            for n in range(group):
                at = chunk * group + n
                slope_of_gates(at, dot(pick(tab, at), unfold(at, yl_buf)), gate_buf, l_buf)
            route_grads(chunk)

        @pl.when(inner)
        def _():
            down(line_g, chunk).wait_recv()

        @pl.when(inner & (chunk == chunks - 1))
        def _():
            sum_pieces()

        arrived(3, chunk, ur_buf)
        for n in range(group):
            at = chunk * group + n
            picked = dot(pick(tab, at), unfold(at, ur_buf))
            grad_u = picked[:tok] + picked[tok:] + dul_buf[at]
            h_wide = h_buf[at].astype(F32)
            inv = inv_rms(h_wide)
            scaled = grad_u * gain_ref[...]
            proj = jnp.mean(scaled * h_wide, axis=-1, keepdims=True)
            grad = g_buf[at].astype(F32) + inv * scaled - h_wide * (inv * inv * inv * proj)
            gs_buf[at] = grad.astype(BF16)
            dul_buf[at] = grad_u

        @pl.when(lower)
        def _():
            for n in range(group):
                at = chunk * group + n
                send_grad(at, gs_buf[at].astype(F32), gatein_buf, tab_in, dn_buf)
            exchange(4, 2, chunk, dn_buf, dr_buf, lambda k: ahead(k, sec - 1), order_all)
            down(line_g, chunk, sec - 1).start()
            for n in range(group):
                at = chunk * group + n
                slope_of_gates(at, pick_buf[at].astype(F32), gatein_buf, ls_buf)
            down(line_l, chunk, sec - 1).start()

        @pl.when(first)
        def _():
            for target in range(1, ns):
                gin_copy(chunk, target).start()
            gin_ref[span(chunk)] = gs_buf[span(chunk), :, 0:part]

        for n in range(group):
            at = chunk * group + n
            h_wide = h_buf[at].astype(F32)
            acc_g[...] += jnp.sum(dul_buf[at] * h_wide * inv_rms(h_wide), axis=0, keepdims=True)

    latest = chunks + LAG - 1
    turn = jnp.minimum(LAG + BETWEEN * (ns - 1 - sec), latest)
    tasks = ((tokens, 0), (experts, LAG), (expert_grads, turn), (grads, turn + LAG))

    def step(i, carry):
        for task, lag in tasks:
            at = i - lag

            @pl.when((at >= 0) & (at < chunks))
            def _():
                task(at)

        return carry

    lax.fori_loop(0, latest + chunks + LAG, step, 0)

    for i in range(ne):
        gain_s[i : i + 1, :] = acc_g[:, i * piece : (i + 1) * piece].astype(BF16)
    for k in order:
        gain_copy(k).start()

    @pl.when(last)
    def _():
        sum_pieces()

    @pl.when(sec != 0)
    def _():
        def take(chunk, carry):
            dst = gin_r.at[span(chunk)]
            pltpu.make_async_copy(dst, dst, gin_recv.at[chunk]).wait()
            return carry

        lax.fori_loop(0, chunks, take, 0)
        gin_ref[...] = gin_r[...]

    sums = sum_r.at[:, pl.ds(0, (ne - 1) * piece)]
    wait_all(sums, red_recv.at[1])
    router_sum_ref[...] = sum_r[...]
    gains = gain_r.at[pl.ds(1, ne - 1)]
    wait_all(gains, red_recv.at[2])
    total = gain_s[...].astype(F32)
    for k in range(1, ne):
        total = total + gain_r[k].astype(F32)
    for i in range(ne):
        gain_sum_ref[:, i * piece : (i + 1) * piece] = total[i : i + 1, :]

    wait_all(part_r.at[pl.ds(1, ne - 1)], red_send.at[0])
    wait_all(sums, red_send.at[1])
    wait_all(gains, red_send.at[2])
    for store in stores:
        store.wait()

    def drain(chunk, carry):
        wait_all(others(xs_buf, chunk), send_sem.at[0, chunk])
        wait_all(others(us_buf, chunk), send_sem.at[3, chunk])

        @pl.when(inner)
        def _():
            wait_all(ys_buf.at[span(chunk)], send_sem.at[1, chunk])
            up(line_h, chunk).wait_send()
            up(line_gate, chunk).wait_send()

        @pl.when(last)
        def _():
            wait_all(others(ys_buf, chunk), send_sem.at[1, chunk])
            wait_all(others(ds_buf, chunk), send_sem.at[2, chunk])

        @pl.when(lower)
        def _():
            wait_all(dn_buf.at[span(chunk)], send_sem.at[4, chunk])
            down(line_g, chunk).wait_send()
            down(line_l, chunk).wait_send()

        @pl.when(first)
        def _():
            for target in range(1, ns):
                gin_copy(chunk, target).wait_send()

        return carry

    lax.fori_loop(0, chunks, drain, 0)

    @pl.when(sec != 0)
    def _():
        gathers[0].wait_send()
        gathers[1].wait_send()

    @pl.when(sec != ns - 1)
    def _():
        gathers[2].wait_send()
        table_copy(0).wait_send()


def weight_grad_kernel(
    steps, rows_ref, q_ref, hid_ref, dyr_ref, gin_ref, router_ref, gain_ref,
    gu_hbm, dn_hbm, gin_out, router_out, gain_out, gu_ref, dn_ref, sem,
):
    def block(lhs, rhs, out, hbm, first, n):
        size = lhs.shape[1] // n

        def copy(i):
            at = pl.ds(pl.multiple_of(i * size, size), size)
            return pltpu.make_async_copy(out.at[at], hbm.at[at], sem.at[first + i])

        def step(i, carry):
            at = pl.ds(pl.multiple_of(i * size, size), size)
            out[at, :] = dot_tn(lhs[:, at], rhs[...])
            copy(i).start()
            return carry

        lax.fori_loop(0, n, step, 0)
        return copy

    gu_copy = block(rows_ref, q_ref, gu_ref, gu_hbm, 0, steps[0])
    dn_copy = block(hid_ref, dyr_ref, dn_ref, dn_hbm, steps[0], steps[1])
    gin_out[...] = gin_ref[...]
    router_out[...] = router_ref[...]
    gain_out[...] = gain_ref[...]
    for i in range(steps[0]):
        gu_copy(i).wait()
    for i in range(steps[1]):
        dn_copy(i).wait()


def local(x_in, cotangent, route_ids, norm_gain, router, w_gate_up, w_down):
    ns, ny, nz = (lax.axis_size(a) for a in ("section", "expert", "dp"))
    micro, tok, part = x_in.shape
    width = part * ns
    ne = ny * nz
    cap = 2 * tok // ne
    cells = ne * cap
    ffw = w_down.shape[2]
    chunks = micro // GROUP
    piece = width // ne
    vmem = pltpu.VMEM
    wire = vmem((micro, cells * width // (2 * LANES), 2 * LANES), BF16)
    rows = vmem((micro, tok, width), BF16)
    dma = pltpu.SemaphoreType.DMA
    stash = (
        ((micro * cells, width), BF16),
        ((micro * cells, 2 * ffw), BF16),
        ((micro * cells, ffw), BF16),
        ((micro * cells, width), BF16),
    )
    scratch = (
        [vmem((width, 2 * ffw), BF16), vmem((ffw, width), BF16)]
        + [vmem(*entry) for entry in stash]
        + [
            vmem((micro, 2 * tok + cells, LANES), BF16),
            vmem((micro, 2 * tok + cells, LANES), BF16),
            vmem((micro, tok, ne), F32),
        ]
        + [rows] * 5
        + [wire] * 10
        + [
            vmem((micro, 2 * tok, width), BF16),
            vmem((micro, 2 * tok, LANES), F32),
            vmem((micro, 2 * tok, LANES), F32),
            vmem((micro, tok, LANES), F32),
            vmem((micro, tok, LANES), F32),
            vmem((micro * cells, ffw), F32),
            vmem((micro * cells, ffw), F32),
            vmem((micro, tok, width), F32),
            vmem((2, cells * width // (2 * LANES), LANES), F32),
            vmem((ne, width), F32),
            vmem((1, width), F32),
            vmem((ne, width), BF16), vmem((ne, ne, piece), BF16),
            vmem((ne, piece), F32), vmem((ne, width), F32),
            vmem((ne, piece), BF16), vmem((ne, ne, piece), BF16),
            vmem((micro, tok, part), BF16),
            dma((5, chunks)), dma((5, chunks)), dma((4, chunks)), dma((4, chunks)), dma((2,)),
            dma((3,)), dma((3,)), dma((ns, chunks)), dma((chunks,)), dma((3,)), dma((3,)), dma((6,)),
        ]
    )
    small = (
        jax.ShapeDtypeStruct((micro, tok, part), BF16),
        jax.ShapeDtypeStruct((ne, width), F32),
        jax.ShapeDtypeStruct((1, width), F32),
    )
    in_vmem = pl.BlockSpec(memory_space=pltpu.VMEM)
    anywhere = pl.BlockSpec(memory_space=pl.ANY)
    *saved, grad_in, sum_router, sum_gain = pl.pallas_call(
        functools.partial(stack_kernel, (ns, ny, nz, cap)),
        out_shape=tuple(jax.ShapeDtypeStruct(*entry) for entry in stash) + small,
        in_specs=[in_vmem] * 5 + [anywhere] * 2,
        out_specs=[anywhere] * 4 + [in_vmem] * 3,
        scratch_shapes=scratch,
        compiler_params=pltpu.CompilerParams(
            collective_id=0, has_side_effects=True, vmem_limit_bytes=60 * 1024 * 1024
        ),
    )(
        x_in, cotangent, jnp.transpose(route_ids[0], (0, 2, 1)), norm_gain, router[0].T,
        w_gate_up[0, 0], w_down[0, 0],
    )
    steps = (width // 256, max(1, ffw // 128))
    grad_gu, grad_dn, grad_in, sum_router, sum_gain = pl.pallas_call(
        functools.partial(weight_grad_kernel, steps),
        out_shape=(
            jax.ShapeDtypeStruct((width, 2 * ffw), F32),
            jax.ShapeDtypeStruct((ffw, width), F32),
        )
        + small,
        in_specs=[in_vmem] * 7,
        out_specs=[anywhere] * 2 + [in_vmem] * 3,
        scratch_shapes=[
            vmem((width, 2 * ffw), F32),
            vmem((ffw, width), F32),
            dma((sum(steps),)),
        ],
        compiler_params=pltpu.CompilerParams(vmem_limit_bytes=40 * 1024 * 1024),
    )(*saved, grad_in, sum_router, sum_gain)
    return grad_in, grad_gu[None, None], grad_dn[None, None], sum_router.T[None], sum_gain


def solution(mesh):
    in_specs = (
        P(None, ("expert", "dp"), "section"),
        P(None, ("expert", "dp"), "section"),
        P("section", None, ("expert", "dp"), None),
        P("section", None),
        P("section", None, None),
        P("section", ("expert", "dp"), None, None),
        P("section", ("expert", "dp"), None, None),
    )
    out_specs = (
        P(None, ("expert", "dp"), "section"),
        P("section", ("expert", "dp"), None, None),
        P("section", ("expert", "dp"), None, None),
        P("section", None, None),
        P("section", None),
    )
    return jax.shard_map(local, mesh=mesh, in_specs=in_specs, out_specs=out_specs, check_vma=False)
```

```python
import functools

import jax
import jax.numpy as jnp
from jax import lax
from jax.experimental import pallas as pl
from jax.experimental.pallas import tpu as pltpu
from jax.sharding import PartitionSpec as P

EPS = 1e-05
GROUP = 1
LAG = 1
BETWEEN = 5
LANES = 128
MESH = pl.DeviceIdType.MESH
F32 = jnp.float32
BF16 = jnp.bfloat16


def dot(lhs, rhs):
    return jnp.dot(lhs, rhs, preferred_element_type=F32)


def dot_nt(lhs, rhs):
    return lax.dot_general(lhs, rhs, (((1,), (1,)), ((), ())), preferred_element_type=F32)


def dot_tn(lhs, rhs):
    return lax.dot_general(lhs, rhs, (((0,), (0,)), ((), ())), preferred_element_type=F32)


def stack_kernel(
    sizes,
    x_ref, cot_ref, route_ref, gain_ref, router_ref, wgu_hbm, wdn_hbm,
    rows_hbm, q_hbm, hid_hbm, dyr_hbm, gin_ref, router_sum_ref, gain_sum_ref,
    wgu_ref, wdn_ref, wgu_t, wdn_t, rows_ref, q_ref, hid_ref, dyr_ref, tab, tab_in, sign_ref,
    h_buf, hin_buf, g_buf, u_buf, gs_buf,
    xs_buf, xr_buf, ys_buf, yr_buf, yl_buf, ds_buf, dn_buf, dr_buf, us_buf, ur_buf,
    pick_buf, gate_buf, gatein_buf, l_buf, ls_buf, slope_buf, silu_buf, dul_buf, wide,
    acc_r, acc_g, part_s, part_r, sum_s, sum_r, gain_s, gain_r, gin_r,
    send_sem, recv_sem, line_send, line_recv, tab_sem, gather_send, gather_recv, gin_send, gin_recv,
    red_send, red_recv, local_sem,
):
    ns, ny, nz, cap = sizes
    ne = ny * nz
    micro, tok, width = h_buf.shape
    part = width // ns
    cells = ne * cap
    blk = cap * (width // (2 * LANES))
    folds = width // (2 * LANES)
    group = GROUP
    chunks = micro // group
    ffw = wdn_ref.shape[0]
    sec = lax.axis_index("section")
    ey = lax.axis_index("expert")
    ez = lax.axis_index("dp")

    first, last = sec == 0, sec == ns - 1
    inner, lower = sec != ns - 1, sec != 0

    def ahead(k, section=None):
        there = {"expert": lax.rem(ey + k // nz, ny), "dp": lax.rem(ez + k % nz, nz)}
        return there if section is None else {"section": section, **there}

    def behind(k, section=None):
        there = {"expert": lax.rem(ey + ny - k // nz, ny), "dp": lax.rem(ez + nz - k % nz, nz)}
        return there if section is None else {"section": section, **there}

    def far(k):
        ky, kz = k // nz, k % nz
        return min(ky, ny - ky) + min(kz, nz - kz)

    order = sorted(range(1, ne), key=lambda k: -far(k))
    order_all = order + [0]

    loads = [
        pltpu.make_async_copy(src, dst, local_sem.at[n])
        for n, (src, dst) in enumerate(((wgu_hbm, wgu_ref), (wdn_hbm, wdn_ref)))
    ]
    stores = [
        pltpu.make_async_copy(src, dst, local_sem.at[2 + n])
        for n, (src, dst) in enumerate(
            ((rows_ref, rows_hbm), (hid_ref, hid_hbm), (dyr_ref, dyr_hbm), (q_ref, q_hbm))
        )
    ]
    for load in loads:
        load.start()

    barrier = pltpu.get_barrier_semaphore()
    for k in range(1, ne):
        pl.semaphore_signal(barrier, inc=1, device_id=ahead(k), device_id_type=MESH)
        for step in (1, ns - 1):
            there = ahead(k, lax.rem(sec + step, ns))
            pl.semaphore_signal(barrier, inc=1, device_id=there, device_id_type=MESH)
    for step in range(1, ns):
        pl.semaphore_signal(
            barrier, inc=1, device_id={"section": lax.rem(sec + step, ns)}, device_id_type=MESH
        )
    pl.semaphore_wait(barrier, 3 * (ne - 1) + ns - 1)

    my_cols = pl.ds(pl.multiple_of(sec * part, LANES), part)

    def gather_copy(which, src, dst, first, count, owner):
        at = pl.ds(first, count)
        return pltpu.make_async_remote_copy(
            src_ref=src.at[at], dst_ref=dst.at[at, :, my_cols],
            send_sem=gather_send.at[which], recv_sem=gather_recv.at[which],
            device_id={"section": owner}, device_id_type=MESH,
        )

    gathers = (
        gather_copy(0, x_ref, h_buf, 0, group, 0),
        gather_copy(1, x_ref, h_buf, group, micro - group, 0),
        gather_copy(2, cot_ref, g_buf, 0, micro, ns - 1),
    )

    @pl.when(sec != 0)
    def _():
        gathers[0].start()
        gathers[1].start()

    @pl.when(sec != ns - 1)
    def _():
        gathers[2].start()

    @pl.when(sec == 0)
    def _():
        h_buf[:, :, 0:part] = x_ref[...]

    @pl.when(sec == ns - 1)
    def _():
        g_buf[:, :, (ns - 1) * part :] = cot_ref[...]

    kinds = lax.broadcasted_iota(jnp.int32, (ne, tok), 0)
    place = jnp.zeros((ne, tok), F32)
    for e in range(ne):
        rel = lax.rem(e // nz + ny - ey, ny) * nz + lax.rem(e % nz + nz - ez, nz)
        place = jnp.where(kinds == e, (rel * cap).astype(F32), place)
    earlier = lax.broadcasted_iota(jnp.int32, (tok, tok), 0)
    earlier = (earlier < lax.broadcasted_iota(jnp.int32, (tok, tok), 1)).astype(BF16)
    cell_ids = lax.broadcasted_iota(jnp.int32, (cells, tok), 0).astype(F32)

    def eye(n):
        rows_id = lax.broadcasted_iota(jnp.int32, (n, n), 0)
        return (rows_id == lax.broadcasted_iota(jnp.int32, (n, n), 1)).astype(BF16)

    def tables(at, carry):
        named = route_ref[at]
        hits = [(kinds == named[k : k + 1, :]).astype(F32) for k in range(2)]
        before = dot((hits[0] + hits[1]).astype(BF16), earlier) + place
        for k in range(2):
            cell = jnp.sum(hits[k] * before, axis=0, keepdims=True)
            tab[at, 2 * tok :, k * tok : (k + 1) * tok] = (cell_ids == cell).astype(BF16)
        turned = dot_nt(eye(2 * tok), tab[at, 2 * tok :, : 2 * tok])
        tab[at, : 2 * tok, :cells] = turned.astype(BF16)
        sign_ref[at] = dot_nt(eye(tok), (hits[0] - hits[1]).astype(BF16))
        return carry

    tab[...] = jnp.zeros_like(tab)
    lax.fori_loop(0, micro, tables, 0)

    def table_copy(target):
        return pltpu.make_async_remote_copy(
            src_ref=tab, dst_ref=tab_in, send_sem=tab_sem.at[0], recv_sem=tab_sem.at[1],
            device_id={"section": target}, device_id_type=MESH,
        )

    @pl.when(inner)
    def _():
        table_copy(sec + 1).start()

    def pick(table, at):
        return table[at, : 2 * tok, :cells]

    def put(table, at):
        return table[at, 2 * tok :, : 2 * tok]

    acc_r[...] = jnp.zeros_like(acc_r)
    acc_g[...] = jnp.zeros_like(acc_g)

    def span(chunk):
        return pl.ds(chunk * group, group)

    def exchange(sent, kind, chunk, src, dst, target, blocks):
        for k in blocks:
            rows = pl.ds(k * blk, blk)
            pltpu.make_async_remote_copy(
                src_ref=src.at[span(chunk), rows], dst_ref=dst.at[span(chunk), rows],
                send_sem=send_sem.at[sent, chunk], recv_sem=recv_sem.at[kind, chunk],
                device_id=target(k), device_id_type=MESH,
            ).start()

    def wait_all(ref, sem):
        pltpu.make_async_copy(ref, ref, sem).wait()

    def others(buf, chunk):
        return buf.at[span(chunk), pl.ds(blk, (ne - 1) * blk)]

    def arrived(kind, chunk, dst):
        wait_all(others(dst, chunk), recv_sem.at[kind, chunk])

    def all_arrived(kind, chunk, dst):
        wait_all(dst.at[span(chunk)], recv_sem.at[kind, chunk])

    def fold(value, at, send, recv=None):
        for j in range(folds):
            for half in range(2):
                left = (2 * j + half) * LANES
                wide[half, pl.ds(j, cells, stride=folds), :] = value[:, left : left + LANES]
        for half in range(2):
            cols = slice(half * LANES, (half + 1) * LANES)
            packed = wide[half].astype(BF16)
            send[at, :, cols] = packed
            if recv is not None:
                recv[at, 0:blk, cols] = packed[0:blk]

    def unfold(at, recv):
        for half in range(2):
            wide[half] = recv[at, :, half * LANES : (half + 1) * LANES].astype(F32)
        pieces = [
            wide[half, pl.ds(j, cells, stride=folds), :] for j in range(folds) for half in range(2)
        ]
        return jnp.concatenate(pieces, axis=1).astype(BF16)

    def line_copy(way, chunk, src, dst, target):
        return pltpu.make_async_remote_copy(
            src_ref=src.at[span(chunk)], dst_ref=dst.at[span(chunk)],
            send_sem=line_send.at[way, chunk], recv_sem=line_recv.at[way, chunk],
            device_id={"section": target}, device_id_type=MESH,
        )

    def inv_rms(h_wide):
        return lax.rsqrt(jnp.mean(h_wide * h_wide, axis=-1, keepdims=True) + EPS)

    def wait_gather(which, dst, first, count):
        part_ref = dst.at[pl.ds(first, count), :, pl.ds(0, (ns - 1) * part)]
        pltpu.make_async_copy(part_ref, part_ref, gather_recv.at[which]).wait()

    line_h, line_gate, line_g, line_l = range(4)

    def up(way, chunk, target=0):
        pair = (h_buf, hin_buf) if way == line_h else (gate_buf, gatein_buf)
        return line_copy(way, chunk, *pair, target)

    def down(way, chunk, target=0):
        pair = (gs_buf, g_buf) if way == line_g else (ls_buf, l_buf)
        return line_copy(way, chunk, *pair, target)

    def turn_weights():
        for src, dst in ((wgu_ref, wgu_t), (wdn_ref, wdn_t)):
            size = min(2 * LANES, src.shape[1])
            one = eye(size)

            def turn(j, carry, src=src, dst=dst, size=size, one=one):
                at = pl.ds(pl.multiple_of(j * size, size), size)
                dst[at, :] = dot_nt(one, src[:, at]).astype(BF16)
                return carry

            lax.fori_loop(0, src.shape[1] // size, turn, 0)

    for load in loads:
        load.wait()

    @pl.when(sec >= ns // 2)
    def _():
        turn_weights()

    def tokens(chunk):
        @pl.when(first & (chunk == 0))
        def _():
            wait_gather(0, h_buf, 0, group)

        @pl.when(first & (chunk == 1))
        def _():
            wait_gather(1, h_buf, group, micro - group)

        @pl.when(lower & (chunk == 0))
        def _():
            table_copy(0).wait_recv()

        @pl.when(lower)
        def _():
            up(line_h, chunk).wait_recv()
            up(line_gate, chunk).wait_recv()
            all_arrived(1, chunk, yr_buf)
            for n in range(group):
                at = chunk * group + n
                picked = dot(pick(tab_in, at), unfold(at, yr_buf))
                gates = gatein_buf[at][:, :1]
                total = gates[:tok] * picked[:tok] + gates[tok:] * picked[tok:]
                h_buf[at] = (hin_buf[at].astype(F32) + total).astype(BF16)
                pick_buf[at] = picked.astype(BF16)

        for n in range(group):
            at = chunk * group + n
            h_wide = h_buf[at].astype(F32)
            normed = (h_wide * inv_rms(h_wide) * gain_ref[...]).astype(BF16)
            u_buf[at] = normed
            both = jnp.concatenate([normed, normed], axis=0)
            fold(dot(put(tab, at), both), at, xs_buf, xr_buf)
        exchange(0, 0, chunk, xs_buf, xr_buf, ahead, order)
        for n in range(group):
            at = chunk * group + n
            logits = dot_nt(u_buf[at], router_ref[...])
            gap = jnp.sum(logits * sign_ref[at], axis=-1, keepdims=True)
            gates = jnp.concatenate([jax.nn.sigmoid(gap), jax.nn.sigmoid(-gap)], axis=0)
            gate_buf[at] = jnp.broadcast_to(gates, (2 * tok, LANES))

        @pl.when(inner)
        def _():
            up(line_h, chunk, sec + 1).start()
            up(line_gate, chunk, sec + 1).start()

        @pl.when(last & (chunk == 0))
        def _():
            wait_gather(2, g_buf, 0, micro)

        @pl.when(last)
        def _():
            for n in range(group):
                at = chunk * group + n
                send_grad(at, g_buf[at].astype(F32), gate_buf, tab, ds_buf, dr_buf)
            exchange(2, 2, chunk, ds_buf, dr_buf, ahead, order)

    def send_grad(at, grad, gate_ref, table, send, recv=None):
        scaled = (jnp.concatenate([grad, grad], axis=0) * gate_ref[at][:, :1]).astype(BF16)
        fold(dot(put(table, at), scaled), at, send, recv)

    def experts(chunk):
        arrived(0, chunk, xr_buf)
        rows = pl.ds(pl.multiple_of(chunk * group * cells, cells), group * cells)
        for n in range(group):
            at = chunk * group + n
            rows_ref[pl.ds(pl.multiple_of(at * cells, cells), cells), :] = unfold(at, xr_buf)
        gate_up = dot(rows_ref[rows, :], wgu_ref[...])
        gate_part = gate_up[:, :ffw]
        up_part = gate_up[:, ffw:]
        sig = jax.nn.sigmoid(gate_part)
        silu = gate_part * sig
        hidden = (silu * up_part).astype(BF16)
        hid_ref[rows, :] = hidden
        out = dot(hidden, wdn_ref[...])
        for n in range(group):
            fold(out[n * cells : (n + 1) * cells], chunk * group + n, ys_buf)

        @pl.when(inner)
        def _():
            exchange(1, 1, chunk, ys_buf, yr_buf, lambda k: behind(k, sec + 1), order_all)

        @pl.when(last)
        def _():
            exchange(1, 4, chunk, ys_buf, yl_buf, behind, order)
            yl_buf[span(chunk), 0:blk] = ys_buf[span(chunk), 0:blk]

        silu_buf[rows, :] = silu
        slope_buf[rows, :] = up_part * (sig * (1.0 + gate_part * (1.0 - sig)))

        @pl.when(chunk == chunks - 1)
        def _():
            stores[0].start()
            stores[1].start()

        @pl.when((chunk == chunks - 1) & (sec < ns // 2))
        def _():
            turn_weights()

    piece = width // ne
    me = ey * nz + ez
    my_piece = pl.ds(pl.multiple_of(me * piece, LANES), piece)

    def part_copy(k):
        there = lax.rem(ey + k // nz, ny) * nz + lax.rem(ez + k % nz, nz)
        return pltpu.make_async_remote_copy(
            src_ref=part_s.at[:, pl.ds(pl.multiple_of(there * piece, LANES), piece)],
            dst_ref=part_r.at[k], send_sem=red_send.at[0], recv_sem=red_recv.at[0],
            device_id=ahead(k), device_id_type=MESH,
        )

    def sum_copy(k):
        return pltpu.make_async_remote_copy(
            src_ref=sum_s, dst_ref=sum_r.at[:, my_piece],
            send_sem=red_send.at[1], recv_sem=red_recv.at[1],
            device_id=ahead(k), device_id_type=MESH,
        )

    def gain_copy(k):
        return pltpu.make_async_remote_copy(
            src_ref=gain_s, dst_ref=gain_r.at[k],
            send_sem=red_send.at[2], recv_sem=red_recv.at[2],
            device_id=ahead(k), device_id_type=MESH,
        )

    def slope_of_gates(at, picked, gate_ref, out):
        gates = gate_ref[at][:, :1]
        grad = (g_buf if out is l_buf else gs_buf)[at].astype(F32)
        diff = jnp.sum(grad * (picked[:tok] - picked[tok:]), axis=-1, keepdims=True)
        out[at] = jnp.broadcast_to(gates[:tok] * gates[tok:] * diff, (tok, LANES))

    def route_grads(chunk):
        for n in range(group):
            at = chunk * group + n
            cols = (l_buf[at][:, :1] * sign_ref[at]).astype(BF16)
            dul_buf[at] = dot(cols, router_ref[...])
            acc_r[...] += dot_tn(cols, u_buf[at])

        @pl.when(chunk == chunks - 1)
        def _():
            part_s[...] = acc_r[...].astype(BF16)
            for k in order:
                part_copy(k).start()

    def sum_pieces():
        wait_all(part_r.at[pl.ds(1, ne - 1)], red_recv.at[0])
        total = part_s[:, my_piece].astype(F32)
        for k in range(1, ne):
            total = total + part_r[k].astype(F32)
        sum_s[...] = total
        sum_r[:, my_piece] = total
        for k in order:
            sum_copy(k).start()

    def expert_grads(chunk):
        @pl.when(inner)
        def _():
            all_arrived(2, chunk, dr_buf)

        @pl.when(last)
        def _():
            arrived(2, chunk, dr_buf)

        rows = pl.ds(pl.multiple_of(chunk * group * cells, cells), group * cells)
        for n in range(group):
            at = chunk * group + n
            dyr_ref[pl.ds(pl.multiple_of(at * cells, cells), cells), :] = unfold(at, dr_buf)
        d_hidden = dot(dyr_ref[rows, :], wdn_t[...])
        q_ref[rows, :ffw] = (d_hidden * slope_buf[rows, :]).astype(BF16)
        q_ref[rows, ffw:] = (d_hidden * silu_buf[rows, :]).astype(BF16)
        out = dot(q_ref[rows, :], wgu_t[...])
        for n in range(group):
            fold(out[n * cells : (n + 1) * cells], chunk * group + n, us_buf, ur_buf)
        exchange(3, 3, chunk, us_buf, ur_buf, behind, order)

        @pl.when(chunk == chunks - 1)
        def _():
            stores[2].start()
            stores[3].start()

        @pl.when(inner)
        def _():
            down(line_l, chunk).wait_recv()
            route_grads(chunk)

    def gin_copy(chunk, target):
        return pltpu.make_async_remote_copy(
            src_ref=gs_buf.at[span(chunk), :, pl.ds(target * part, part)],
            dst_ref=gin_r.at[span(chunk)],
            send_sem=gin_send.at[target, chunk], recv_sem=gin_recv.at[chunk],
            device_id={"section": target}, device_id_type=MESH,
        )

    def grads(chunk):
        @pl.when(last)
        def _():
            arrived(4, chunk, yl_buf)
            for n in range(group):
                at = chunk * group + n
                slope_of_gates(at, dot(pick(tab, at), unfold(at, yl_buf)), gate_buf, l_buf)
            route_grads(chunk)

        @pl.when(inner)
        def _():
            down(line_g, chunk).wait_recv()

        @pl.when(inner & (chunk == chunks - 1))
        def _():
            sum_pieces()

        arrived(3, chunk, ur_buf)
        for n in range(group):
            at = chunk * group + n
            picked = dot(pick(tab, at), unfold(at, ur_buf))
            grad_u = picked[:tok] + picked[tok:] + dul_buf[at]
            h_wide = h_buf[at].astype(F32)
            inv = inv_rms(h_wide)
            scaled = grad_u * gain_ref[...]
            proj = jnp.mean(scaled * h_wide, axis=-1, keepdims=True)
            grad = g_buf[at].astype(F32) + inv * scaled - h_wide * (inv * inv * inv * proj)
            gs_buf[at] = grad.astype(BF16)
            dul_buf[at] = grad_u

        @pl.when(lower)
        def _():
            for n in range(group):
                at = chunk * group + n
                send_grad(at, gs_buf[at].astype(F32), gatein_buf, tab_in, dn_buf)
            exchange(4, 2, chunk, dn_buf, dr_buf, lambda k: ahead(k, sec - 1), order_all)
            down(line_g, chunk, sec - 1).start()
            for n in range(group):
                at = chunk * group + n
                slope_of_gates(at, pick_buf[at].astype(F32), gatein_buf, ls_buf)
            down(line_l, chunk, sec - 1).start()

        @pl.when(first)
        def _():
            for target in range(1, ns):
                gin_copy(chunk, target).start()
            gin_ref[span(chunk)] = gs_buf[span(chunk), :, 0:part]

        for n in range(group):
            at = chunk * group + n
            h_wide = h_buf[at].astype(F32)
            acc_g[...] += jnp.sum(dul_buf[at] * h_wide * inv_rms(h_wide), axis=0, keepdims=True)

    latest = chunks + LAG - 1
    turn = jnp.minimum(LAG + BETWEEN * (ns - 1 - sec), latest)
    tasks = ((tokens, 0), (experts, LAG), (expert_grads, turn), (grads, turn + LAG))

    def step(i, carry):
        for task, lag in tasks:
            at = i - lag

            @pl.when((at >= 0) & (at < chunks))
            def _():
                task(at)

        return carry

    lax.fori_loop(0, latest + chunks + LAG, step, 0)

    for i in range(ne):
        gain_s[i : i + 1, :] = acc_g[:, i * piece : (i + 1) * piece].astype(BF16)
    for k in order:
        gain_copy(k).start()

    @pl.when(last)
    def _():
        sum_pieces()

    @pl.when(sec != 0)
    def _():
        def take(chunk, carry):
            dst = gin_r.at[span(chunk)]
            pltpu.make_async_copy(dst, dst, gin_recv.at[chunk]).wait()
            return carry

        lax.fori_loop(0, chunks, take, 0)
        gin_ref[...] = gin_r[...]

    sums = sum_r.at[:, pl.ds(0, (ne - 1) * piece)]
    wait_all(sums, red_recv.at[1])
    router_sum_ref[...] = sum_r[...]
    gains = gain_r.at[pl.ds(1, ne - 1)]
    wait_all(gains, red_recv.at[2])
    total = gain_s[...].astype(F32)
    for k in range(1, ne):
        total = total + gain_r[k].astype(F32)
    for i in range(ne):
        gain_sum_ref[:, i * piece : (i + 1) * piece] = total[i : i + 1, :]

    wait_all(part_r.at[pl.ds(1, ne - 1)], red_send.at[0])
    wait_all(sums, red_send.at[1])
    wait_all(gains, red_send.at[2])
    for store in stores:
        store.wait()

    def drain(chunk, carry):
        wait_all(others(xs_buf, chunk), send_sem.at[0, chunk])
        wait_all(others(us_buf, chunk), send_sem.at[3, chunk])

        @pl.when(inner)
        def _():
            wait_all(ys_buf.at[span(chunk)], send_sem.at[1, chunk])
            up(line_h, chunk).wait_send()
            up(line_gate, chunk).wait_send()

        @pl.when(last)
        def _():
            wait_all(others(ys_buf, chunk), send_sem.at[1, chunk])
            wait_all(others(ds_buf, chunk), send_sem.at[2, chunk])

        @pl.when(lower)
        def _():
            wait_all(dn_buf.at[span(chunk)], send_sem.at[4, chunk])
            down(line_g, chunk).wait_send()
            down(line_l, chunk).wait_send()

        @pl.when(first)
        def _():
            for target in range(1, ns):
                gin_copy(chunk, target).wait_send()

        return carry

    lax.fori_loop(0, chunks, drain, 0)

    @pl.when(sec != 0)
    def _():
        gathers[0].wait_send()
        gathers[1].wait_send()

    @pl.when(sec != ns - 1)
    def _():
        gathers[2].wait_send()
        table_copy(0).wait_send()


def weight_grad_kernel(
    steps, rows_hbm, q_hbm, hid_hbm, dyr_hbm, gin_hbm, router_hbm, gain_hbm,
    gu_hbm, dn_hbm, gin_out, router_out, gain_out,
    rows_ref, q_ref, hid_ref, dyr_ref, gin_ref, router_ref, gain_ref, gu_ref, dn_ref, sem, load_sem, pass_sem,
):
    sources = (rows_hbm, q_hbm, hid_hbm, dyr_hbm, gin_hbm, router_hbm, gain_hbm)
    landings = (rows_ref, q_ref, hid_ref, dyr_ref, gin_ref, router_ref, gain_ref)
    loads = [
        pltpu.make_async_copy(src, dst, load_sem.at[n])
        for n, (src, dst) in enumerate(zip(sources, landings))
    ]
    passes = [
        pltpu.make_async_copy(src, dst, pass_sem.at[n])
        for n, (src, dst) in enumerate(zip(landings[4:], (gin_out, router_out, gain_out)))
    ]
    for load in loads:
        load.start()

    def block(lhs, rhs, out, hbm, first, n):
        size = lhs.shape[1] // n

        def copy(i):
            at = pl.ds(pl.multiple_of(i * size, size), size)
            return pltpu.make_async_copy(out.at[at], hbm.at[at], sem.at[first + i])

        def step(i, carry):
            at = pl.ds(pl.multiple_of(i * size, size), size)
            out[at, :] = dot_tn(lhs[:, at], rhs[...])
            copy(i).start()
            return carry

        lax.fori_loop(0, n, step, 0)
        return copy

    loads[0].wait()
    loads[1].wait()
    gu_copy = block(rows_ref, q_ref, gu_ref, gu_hbm, 0, steps[0])
    for load in loads[2:]:
        load.wait()
    for onward in passes:
        onward.start()
    dn_copy = block(hid_ref, dyr_ref, dn_ref, dn_hbm, steps[0], steps[1])
    for i in range(steps[0]):
        gu_copy(i).wait()
    for i in range(steps[1]):
        dn_copy(i).wait()
    for onward in passes:
        onward.wait()


def local(x_in, cotangent, route_ids, norm_gain, router, w_gate_up, w_down):
    ns, ny, nz = (lax.axis_size(a) for a in ("section", "expert", "dp"))
    micro, tok, part = x_in.shape
    width = part * ns
    ne = ny * nz
    cap = 2 * tok // ne
    cells = ne * cap
    ffw = w_down.shape[2]
    chunks = micro // GROUP
    piece = width // ne
    vmem = pltpu.VMEM
    wire = vmem((micro, cells * width // (2 * LANES), 2 * LANES), BF16)
    rows = vmem((micro, tok, width), BF16)
    dma = pltpu.SemaphoreType.DMA
    stash = (
        ((micro * cells, width), BF16),
        ((micro * cells, 2 * ffw), BF16),
        ((micro * cells, ffw), BF16),
        ((micro * cells, width), BF16),
    )
    scratch = (
        [vmem((width, 2 * ffw), BF16), vmem((ffw, width), BF16)]
        + [vmem((2 * ffw, width), BF16), vmem((width, ffw), BF16)]
        + [vmem(*entry) for entry in stash]
        + [
            vmem((micro, 2 * tok + cells, LANES), BF16),
            vmem((micro, 2 * tok + cells, LANES), BF16),
            vmem((micro, tok, ne), F32),
        ]
        + [rows] * 5
        + [wire] * 10
        + [
            vmem((micro, 2 * tok, width), BF16),
            vmem((micro, 2 * tok, LANES), F32),
            vmem((micro, 2 * tok, LANES), F32),
            vmem((micro, tok, LANES), F32),
            vmem((micro, tok, LANES), F32),
            vmem((micro * cells, ffw), F32),
            vmem((micro * cells, ffw), F32),
            vmem((micro, tok, width), F32),
            vmem((2, cells * width // (2 * LANES), LANES), F32),
            vmem((ne, width), F32),
            vmem((1, width), F32),
            vmem((ne, width), BF16), vmem((ne, ne, piece), BF16),
            vmem((ne, piece), F32), vmem((ne, width), F32),
            vmem((ne, piece), BF16), vmem((ne, ne, piece), BF16),
            vmem((micro, tok, part), BF16),
            dma((5, chunks)), dma((5, chunks)), dma((4, chunks)), dma((4, chunks)), dma((2,)),
            dma((3,)), dma((3,)), dma((ns, chunks)), dma((chunks,)), dma((3,)), dma((3,)), dma((6,)),
        ]
    )
    small = (
        jax.ShapeDtypeStruct((micro, tok, part), BF16),
        jax.ShapeDtypeStruct((ne, width), F32),
        jax.ShapeDtypeStruct((1, width), F32),
    )
    in_vmem = pl.BlockSpec(memory_space=pltpu.VMEM)
    anywhere = pl.BlockSpec(memory_space=pl.ANY)
    *saved, grad_in, sum_router, sum_gain = pl.pallas_call(
        functools.partial(stack_kernel, (ns, ny, nz, cap)),
        out_shape=tuple(jax.ShapeDtypeStruct(*entry) for entry in stash) + small,
        in_specs=[in_vmem] * 5 + [anywhere] * 2,
        out_specs=[anywhere] * 4 + [in_vmem] * 3,
        scratch_shapes=scratch,
        compiler_params=pltpu.CompilerParams(
            collective_id=0, has_side_effects=True, vmem_limit_bytes=60 * 1024 * 1024
        ),
    )(
        x_in, cotangent, jnp.transpose(route_ids[0], (0, 2, 1)), norm_gain, router[0].T,
        w_gate_up[0, 0], w_down[0, 0],
    )
    steps = (width // 256, max(1, ffw // 128))
    grad_gu, grad_dn, grad_in, sum_router, sum_gain = pl.pallas_call(
        functools.partial(weight_grad_kernel, steps),
        out_shape=(
            jax.ShapeDtypeStruct((width, 2 * ffw), F32),
            jax.ShapeDtypeStruct((ffw, width), F32),
        )
        + small,
        in_specs=[anywhere] * 7,
        out_specs=[anywhere] * 5,
        scratch_shapes=[vmem(*entry) for entry in stash]
        + [vmem(entry.shape, entry.dtype) for entry in small]
        + [
            vmem((width, 2 * ffw), F32),
            vmem((ffw, width), F32),
            dma((sum(steps),)),
            dma((7,)),
            dma((3,)),
        ],
        compiler_params=pltpu.CompilerParams(vmem_limit_bytes=60 * 1024 * 1024),
    )(*saved, grad_in, sum_router, sum_gain)
    return grad_in, grad_gu[None, None], grad_dn[None, None], sum_router.T[None], sum_gain


def solution(mesh):
    in_specs = (
        P(None, ("expert", "dp"), "section"),
        P(None, ("expert", "dp"), "section"),
        P("section", None, ("expert", "dp"), None),
        P("section", None),
        P("section", None, None),
        P("section", ("expert", "dp"), None, None),
        P("section", ("expert", "dp"), None, None),
    )
    out_specs = (
        P(None, ("expert", "dp"), "section"),
        P("section", ("expert", "dp"), None, None),
        P("section", ("expert", "dp"), None, None),
        P("section", None, None),
        P("section", None),
    )
    return jax.shard_map(local, mesh=mesh, in_specs=in_specs, out_specs=out_specs, check_vma=False)
```

```python
import functools

import jax
import jax.numpy as jnp
from jax import lax
from jax.experimental import pallas as pl
from jax.experimental.pallas import tpu as pltpu
from jax.sharding import PartitionSpec as P

EPS = 1e-05
GROUP = 1
LAG = 1
BETWEEN = 6
STEPS = (8, 4)
LANES = 128
MESH = pl.DeviceIdType.MESH
F32 = jnp.float32
BF16 = jnp.bfloat16


def dot(lhs, rhs):
    return jnp.dot(lhs, rhs, preferred_element_type=F32)


def dot_nt(lhs, rhs):
    return lax.dot_general(lhs, rhs, (((1,), (1,)), ((), ())), preferred_element_type=F32)


def dot_tn(lhs, rhs):
    return lax.dot_general(lhs, rhs, (((0,), (0,)), ((), ())), preferred_element_type=F32)


def stack_kernel(
    sizes,
    x_hbm, cot_hbm, route_hbm, gain_hbm, router_hbm, wgu_hbm, wdn_hbm,
    rows_hbm, q_hbm, hid_hbm, dyr_hbm, gin_hbm, router_sum_hbm, gain_sum_hbm,
    x_ref, cot_ref, route_ref, gain_ref, router_ref, gin_ref, gain_sum_ref,
    wgu_ref, wdn_ref, wgu_t, wdn_t, rows_ref, q_ref, hid_ref, dyr_ref, tab, tab_in, sign_ref,
    h_buf, hin_buf, g_buf, u_buf, gs_buf,
    xs_buf, xr_buf, ys_buf, yr_buf, ds_buf, dn_buf, dr_buf, us_buf, ur_buf,
    sv_buf, sr_buf, cell_buf, pick_buf, inv_buf, gate_buf, gatein_buf, l_buf, ls_buf, slope_buf, silu_buf, dul_buf, wide,
    acc_r, acc_g, part_s, part_r, sum_s, sum_r, gain_s, gain_r, gin_r,
    send_sem, recv_sem, line_send, line_recv, tab_sem, gather_send, gather_recv, gin_send, gin_recv,
    red_send, red_recv, local_sem,
):
    ns, ny, nz, cap = sizes
    ne = ny * nz
    micro, tok, width = h_buf.shape
    part = width // ns
    cells = ne * cap
    blk = cap * (width // (2 * LANES))
    folds = width // (2 * LANES)
    group = GROUP
    chunks = micro // group
    ffw = wdn_ref.shape[0]
    sec = lax.axis_index("section")
    ey = lax.axis_index("expert")
    ez = lax.axis_index("dp")

    first, last = sec == 0, sec == ns - 1
    inner, lower = sec != ns - 1, sec != 0

    def ahead(k, section=None):
        there = {"expert": lax.rem(ey + k // nz, ny), "dp": lax.rem(ez + k % nz, nz)}
        return there if section is None else {"section": section, **there}

    def behind(k, section=None):
        there = {"expert": lax.rem(ey + ny - k // nz, ny), "dp": lax.rem(ez + nz - k % nz, nz)}
        return there if section is None else {"section": section, **there}

    def far(k):
        ky, kz = k // nz, k % nz
        return min(ky, ny - ky) + min(kz, nz - kz)

    order = sorted(range(1, ne), key=lambda k: -far(k))
    order_all = order + [0]

    loads = [
        pltpu.make_async_copy(src, dst, local_sem.at[n])
        for n, (src, dst) in enumerate(((wgu_hbm, wgu_ref), (wdn_hbm, wdn_ref)))
    ]
    smalls = [
        pltpu.make_async_copy(src, dst, local_sem.at[6 + n])
        for n, (src, dst) in enumerate(
            (
                (x_hbm, x_ref), (cot_hbm, cot_ref), (route_hbm, route_ref),
                (gain_hbm, gain_ref), (router_hbm, router_ref),
            )
        )
    ]
    results = [
        pltpu.make_async_copy(src, dst, local_sem.at[11 + n])
        for n, (src, dst) in enumerate(
            ((sum_r, router_sum_hbm), (gin_ref, gin_hbm), (gain_sum_ref, gain_sum_hbm))
        )
    ]
    stores = [
        pltpu.make_async_copy(src, dst, local_sem.at[2 + n])
        for n, (src, dst) in enumerate(
            ((rows_ref, rows_hbm), (hid_ref, hid_hbm), (dyr_ref, dyr_hbm), (q_ref, q_hbm))
        )
    ]
    for load in smalls + loads:
        load.start()

    barrier = pltpu.get_barrier_semaphore()
    for k in range(1, ne):
        pl.semaphore_signal(barrier, inc=1, device_id=ahead(k), device_id_type=MESH)
        for step in (1, ns - 1):
            there = ahead(k, lax.rem(sec + step, ns))
            pl.semaphore_signal(barrier, inc=1, device_id=there, device_id_type=MESH)
    for step in range(1, ns):
        pl.semaphore_signal(
            barrier, inc=1, device_id={"section": lax.rem(sec + step, ns)}, device_id_type=MESH
        )
    for load in smalls:
        load.wait()
    pl.semaphore_wait(barrier, 3 * (ne - 1) + ns - 1)

    my_cols = pl.ds(pl.multiple_of(sec * part, LANES), part)

    def gather_copy(which, src, dst, first, count, owner):
        at = pl.ds(first, count)
        return pltpu.make_async_remote_copy(
            src_ref=src.at[at], dst_ref=dst.at[at, :, my_cols],
            send_sem=gather_send.at[which], recv_sem=gather_recv.at[which],
            device_id={"section": owner}, device_id_type=MESH,
        )

    gathers = (
        gather_copy(0, x_ref, h_buf, 0, group, 0),
        gather_copy(1, x_ref, h_buf, group, micro - group, 0),
        gather_copy(2, cot_ref, g_buf, 0, micro, ns - 1),
    )

    @pl.when(sec != 0)
    def _():
        gathers[0].start()
        gathers[1].start()

    @pl.when(sec != ns - 1)
    def _():
        gathers[2].start()

    @pl.when(sec == 0)
    def _():
        h_buf[:, :, 0:part] = x_ref[...]

    @pl.when(sec == ns - 1)
    def _():
        g_buf[:, :, (ns - 1) * part :] = cot_ref[...]

    kinds = lax.broadcasted_iota(jnp.int32, (ne, tok), 0)
    place = jnp.zeros((ne, tok), F32)
    for e in range(ne):
        rel = lax.rem(e // nz + ny - ey, ny) * nz + lax.rem(e % nz + nz - ez, nz)
        place = jnp.where(kinds == e, (rel * cap).astype(F32), place)
    earlier = lax.broadcasted_iota(jnp.int32, (tok, tok), 0)
    earlier = (earlier < lax.broadcasted_iota(jnp.int32, (tok, tok), 1)).astype(BF16)
    cell_ids = lax.broadcasted_iota(jnp.int32, (cells, tok), 0).astype(F32)

    def eye(n):
        rows_id = lax.broadcasted_iota(jnp.int32, (n, n), 0)
        return (rows_id == lax.broadcasted_iota(jnp.int32, (n, n), 1)).astype(BF16)

    def tables(at, carry):
        named = route_ref[at]
        hits = [(kinds == named[k : k + 1, :]).astype(F32) for k in range(2)]
        before = dot((hits[0] + hits[1]).astype(BF16), earlier) + place
        for k in range(2):
            cell = jnp.sum(hits[k] * before, axis=0, keepdims=True)
            tab[at, 2 * tok :, k * tok : (k + 1) * tok] = (cell_ids == cell).astype(BF16)
        turned = dot_nt(eye(2 * tok), tab[at, 2 * tok :, : 2 * tok])
        tab[at, : 2 * tok, :cells] = turned.astype(BF16)
        sign_ref[at] = dot_nt(eye(tok), (hits[0] - hits[1]).astype(BF16))
        return carry

    tab[...] = jnp.zeros_like(tab)
    lax.fori_loop(0, micro, tables, 0)

    def table_copy(target):
        return pltpu.make_async_remote_copy(
            src_ref=tab, dst_ref=tab_in, send_sem=tab_sem.at[0], recv_sem=tab_sem.at[1],
            device_id={"section": target}, device_id_type=MESH,
        )

    @pl.when(inner)
    def _():
        table_copy(sec + 1).start()

    def pick(table, at):
        return table[at, : 2 * tok, :cells]

    def put(table, at):
        return table[at, 2 * tok :, : 2 * tok]

    acc_r[...] = jnp.zeros_like(acc_r)
    sv_buf[...] = jnp.zeros_like(sv_buf)
    acc_g[...] = jnp.zeros_like(acc_g)

    def span(chunk):
        return pl.ds(chunk * group, group)

    def exchange(sent, kind, chunk, src, dst, target, blocks):
        for k in blocks:
            rows = pl.ds(k * blk, blk)
            pltpu.make_async_remote_copy(
                src_ref=src.at[span(chunk), rows], dst_ref=dst.at[span(chunk), rows],
                send_sem=send_sem.at[sent, chunk], recv_sem=recv_sem.at[kind, chunk],
                device_id=target(k), device_id_type=MESH,
            ).start()

    def wait_all(ref, sem):
        pltpu.make_async_copy(ref, ref, sem).wait()

    def others(buf, chunk):
        return buf.at[span(chunk), pl.ds(blk, (ne - 1) * blk)]

    def arrived(kind, chunk, dst):
        wait_all(others(dst, chunk), recv_sem.at[kind, chunk])

    def all_arrived(kind, chunk, dst):
        wait_all(dst.at[span(chunk)], recv_sem.at[kind, chunk])

    def fold(value, at, send, recv=None):
        for j in range(folds):
            for half in range(2):
                left = (2 * j + half) * LANES
                wide[half, pl.ds(j, cells, stride=folds), :] = value[:, left : left + LANES]
        for half in range(2):
            cols = slice(half * LANES, (half + 1) * LANES)
            packed = wide[half].astype(BF16)
            send[at, :, cols] = packed
            if recv is not None:
                recv[at, 0:blk, cols] = packed[0:blk]

    def unfold(at, recv):
        for half in range(2):
            wide[half] = recv[at, :, half * LANES : (half + 1) * LANES].astype(F32)
        pieces = [
            wide[half, pl.ds(j, cells, stride=folds), :] for j in range(folds) for half in range(2)
        ]
        return jnp.concatenate(pieces, axis=1).astype(BF16)

    def line_copy(way, chunk, src, dst, target):
        return pltpu.make_async_remote_copy(
            src_ref=src.at[span(chunk)], dst_ref=dst.at[span(chunk)],
            send_sem=line_send.at[way, chunk], recv_sem=line_recv.at[way, chunk],
            device_id={"section": target}, device_id_type=MESH,
        )

    def inv_rms(h_wide):
        return lax.rsqrt(jnp.mean(h_wide * h_wide, axis=-1, keepdims=True) + EPS)

    def wait_gather(which, dst, first, count):
        part_ref = dst.at[pl.ds(first, count), :, pl.ds(0, (ns - 1) * part)]
        pltpu.make_async_copy(part_ref, part_ref, gather_recv.at[which]).wait()

    line_h, line_gate, line_g, line_l = range(4)

    def up(way, chunk, target=0):
        pair = (h_buf, hin_buf) if way == line_h else (gate_buf, gatein_buf)
        return line_copy(way, chunk, *pair, target)

    def down(way, chunk, target=0):
        pair = (gs_buf, g_buf) if way == line_g else (ls_buf, l_buf)
        return line_copy(way, chunk, *pair, target)

    def turn_weights():
        for src, dst in ((wgu_ref, wgu_t), (wdn_ref, wdn_t)):
            size = min(2 * LANES, src.shape[1])
            one = eye(size)

            def turn(j, carry, src=src, dst=dst, size=size, one=one):
                at = pl.ds(pl.multiple_of(j * size, size), size)
                dst[at, :] = dot_nt(one, src[:, at]).astype(BF16)
                return carry

            lax.fori_loop(0, src.shape[1] // size, turn, 0)

    for load in loads:
        load.wait()

    @pl.when(sec >= ns // 2)
    def _():
        turn_weights()

    def tokens(chunk):
        @pl.when(first & (chunk == 0))
        def _():
            wait_gather(0, h_buf, 0, group)

        @pl.when(first & (chunk == 1))
        def _():
            wait_gather(1, h_buf, group, micro - group)

        @pl.when(lower & (chunk == 0))
        def _():
            table_copy(0).wait_recv()

        @pl.when(lower)
        def _():
            up(line_h, chunk).wait_recv()
            up(line_gate, chunk).wait_recv()
            all_arrived(1, chunk, yr_buf)
            for n in range(group):
                at = chunk * group + n
                picked = dot(pick(tab_in, at), unfold(at, yr_buf))
                gates = gatein_buf[at][:, :1]
                total = gates[:tok] * picked[:tok] + gates[tok:] * picked[tok:]
                h_buf[at] = (hin_buf[at].astype(F32) + total).astype(BF16)
                pick_buf[at] = picked.astype(BF16)

        for n in range(group):
            at = chunk * group + n
            h_wide = h_buf[at].astype(F32)
            inv = inv_rms(h_wide)
            normed = (h_wide * inv * gain_ref[...]).astype(BF16)
            inv_buf[at] = jnp.broadcast_to(inv, (tok, LANES))
            u_buf[at] = normed
            both = jnp.concatenate([normed, normed], axis=0)
            fold(dot(put(tab, at), both), at, xs_buf, xr_buf)
        exchange(0, 0, chunk, xs_buf, xr_buf, ahead, order)
        for n in range(group):
            at = chunk * group + n
            logits = dot_nt(u_buf[at], router_ref[...])
            gap = jnp.sum(logits * sign_ref[at], axis=-1, keepdims=True)
            gates = jnp.concatenate([jax.nn.sigmoid(gap), jax.nn.sigmoid(-gap)], axis=0)
            gate_buf[at] = jnp.broadcast_to(gates, (2 * tok, LANES))

        @pl.when(inner)
        def _():
            up(line_h, chunk, sec + 1).start()
            up(line_gate, chunk, sec + 1).start()

        @pl.when(last & (chunk == 0))
        def _():
            wait_gather(2, g_buf, 0, micro)

        @pl.when(last)
        def _():
            for n in range(group):
                at = chunk * group + n
                send_grad(at, g_buf[at].astype(F32), gate_buf, tab, ds_buf, dr_buf)
            exchange(2, 2, chunk, ds_buf, dr_buf, ahead, order)

    def send_grad(at, grad, gate_ref, table, send, recv=None):
        scaled = (jnp.concatenate([grad, grad], axis=0) * gate_ref[at][:, :1]).astype(BF16)
        fold(dot(put(table, at), scaled), at, send, recv)

    def experts(chunk):
        arrived(0, chunk, xr_buf)
        rows = pl.ds(pl.multiple_of(chunk * group * cells, cells), group * cells)
        for n in range(group):
            at = chunk * group + n
            rows_ref[pl.ds(pl.multiple_of(at * cells, cells), cells), :] = unfold(at, xr_buf)
        gate_up = dot(rows_ref[rows, :], wgu_ref[...])
        gate_part = gate_up[:, :ffw]
        up_part = gate_up[:, ffw:]
        sig = jax.nn.sigmoid(gate_part)
        silu = gate_part * sig
        hidden = (silu * up_part).astype(BF16)
        hid_ref[rows, :] = hidden

        @pl.when(inner)
        def _():
            out = dot(hid_ref[rows, :], wdn_ref[...])
            for n in range(group):
                fold(out[n * cells : (n + 1) * cells], chunk * group + n, ys_buf)
            exchange(1, 1, chunk, ys_buf, yr_buf, lambda k: behind(k, sec + 1), order_all)

        silu_buf[rows, :] = silu
        slope_buf[rows, :] = up_part * (sig * (1.0 + gate_part * (1.0 - sig)))

        @pl.when(chunk == chunks - 1)
        def _():
            stores[0].start()
            stores[1].start()

        @pl.when((chunk == chunks - 1) & (sec < ns // 2))
        def _():
            turn_weights()

    piece = width // ne
    me = ey * nz + ez
    my_piece = pl.ds(pl.multiple_of(me * piece, LANES), piece)

    def part_copy(k):
        there = lax.rem(ey + k // nz, ny) * nz + lax.rem(ez + k % nz, nz)
        return pltpu.make_async_remote_copy(
            src_ref=part_s.at[:, pl.ds(pl.multiple_of(there * piece, LANES), piece)],
            dst_ref=part_r.at[k], send_sem=red_send.at[0], recv_sem=red_recv.at[0],
            device_id=ahead(k), device_id_type=MESH,
        )

    def sum_copy(k):
        return pltpu.make_async_remote_copy(
            src_ref=sum_s, dst_ref=sum_r.at[:, my_piece],
            send_sem=red_send.at[1], recv_sem=red_recv.at[1],
            device_id=ahead(k), device_id_type=MESH,
        )

    def gain_copy(k):
        return pltpu.make_async_remote_copy(
            src_ref=gain_s, dst_ref=gain_r.at[k],
            send_sem=red_send.at[2], recv_sem=red_recv.at[2],
            device_id=ahead(k), device_id_type=MESH,
        )

    def slope_of_gates(at):
        picked = pick_buf[at].astype(F32)
        gates = gatein_buf[at][:, :1]
        grad = gs_buf[at].astype(F32)
        diff = jnp.sum(grad * (picked[:tok] - picked[tok:]), axis=-1, keepdims=True)
        ls_buf[at] = jnp.broadcast_to(gates[:tok] * gates[tok:] * diff, (tok, LANES))

    def route_grads(chunk):
        for n in range(group):
            at = chunk * group + n
            cols = (l_buf[at][:, :1] * sign_ref[at]).astype(BF16)
            dul_buf[at] = dot(cols, router_ref[...])
            acc_r[...] += dot_tn(cols, u_buf[at])

        @pl.when(chunk == chunks - 1)
        def _():
            part_s[...] = acc_r[...].astype(BF16)
            for k in order:
                part_copy(k).start()

    def sum_pieces():
        wait_all(part_r.at[pl.ds(1, ne - 1)], red_recv.at[0])
        total = part_s[:, my_piece].astype(F32)
        for k in range(1, ne):
            total = total + part_r[k].astype(F32)
        sum_s[...] = total
        sum_r[:, my_piece] = total
        for k in order:
            sum_copy(k).start()

    def scalar_copy(k, chunk):
        rows = pl.ds(8 * k, 8)
        return pltpu.make_async_remote_copy(
            src_ref=sv_buf.at[span(chunk), rows], dst_ref=sr_buf.at[span(chunk), rows],
            send_sem=send_sem.at[1, chunk], recv_sem=recv_sem.at[4, chunk],
            device_id=behind(k), device_id_type=MESH,
        )

    def other_scalars(buf, chunk):
        return buf.at[span(chunk), pl.ds(8, (ne - 1) * 8)]

    def expert_grads(chunk):
        @pl.when(inner)
        def _():
            all_arrived(2, chunk, dr_buf)

        @pl.when(last)
        def _():
            arrived(2, chunk, dr_buf)

        rows = pl.ds(pl.multiple_of(chunk * group * cells, cells), group * cells)
        for n in range(group):
            at = chunk * group + n
            dyr_ref[pl.ds(pl.multiple_of(at * cells, cells), cells), :] = unfold(at, dr_buf)
        d_hidden = dot(dyr_ref[rows, :], wdn_t[...])

        @pl.when(last)
        def _():
            both = hid_ref[rows, :].astype(F32) * d_hidden
            for n in range(group):
                at = chunk * group + n
                mine = jnp.sum(both[n * cells : (n + 1) * cells], axis=-1, keepdims=True)
                cell_buf[...] = jnp.broadcast_to(mine, (cells, LANES))
                for r in range(cap):
                    sv_buf[at, pl.ds(r, ne, stride=8), :] = cell_buf[pl.ds(r, ne, stride=cap), :]
                sr_buf[at, 0:8] = sv_buf[at, 0:8]
            for k in order:
                scalar_copy(k, chunk).start()

        q_ref[rows, :ffw] = (d_hidden * slope_buf[rows, :]).astype(BF16)
        q_ref[rows, ffw:] = (d_hidden * silu_buf[rows, :]).astype(BF16)
        out = dot(q_ref[rows, :], wgu_t[...])
        for n in range(group):
            fold(out[n * cells : (n + 1) * cells], chunk * group + n, us_buf, ur_buf)
        exchange(3, 3, chunk, us_buf, ur_buf, behind, order)

        @pl.when(chunk == chunks - 1)
        def _():
            stores[2].start()
            stores[3].start()

        @pl.when(inner)
        def _():
            down(line_l, chunk).wait_recv()
            route_grads(chunk)

    def gin_copy(chunk, target):
        return pltpu.make_async_remote_copy(
            src_ref=gs_buf.at[span(chunk), :, pl.ds(target * part, part)],
            dst_ref=gin_r.at[span(chunk)],
            send_sem=gin_send.at[target, chunk], recv_sem=gin_recv.at[chunk],
            device_id={"section": target}, device_id_type=MESH,
        )

    def grads(chunk):
        @pl.when(last)
        def _():
            wait_all(other_scalars(sr_buf, chunk), recv_sem.at[4, chunk])
            for n in range(group):
                at = chunk * group + n
                for r in range(cap):
                    cell_buf[pl.ds(r, ne, stride=cap), :] = sr_buf[at, pl.ds(r, ne, stride=8), :]
                value = cell_buf[...]
                high = value.astype(BF16)
                low = (value - high.astype(F32)).astype(BF16)
                picked = dot(pick(tab, at), high) + dot(pick(tab, at), low)
                gates = gate_buf[at]
                l_buf[at] = gates[tok:] * picked[:tok] - gates[:tok] * picked[tok:]
            route_grads(chunk)

        @pl.when(inner)
        def _():
            down(line_g, chunk).wait_recv()

        @pl.when(inner & (chunk == chunks - 1))
        def _():
            sum_pieces()

        arrived(3, chunk, ur_buf)
        for n in range(group):
            at = chunk * group + n
            picked = dot(pick(tab, at), unfold(at, ur_buf))
            grad_u = picked[:tok] + picked[tok:] + dul_buf[at]
            h_wide = h_buf[at].astype(F32)
            inv = inv_buf[at][:, :1]
            scaled = grad_u * gain_ref[...]
            proj = jnp.mean(scaled * h_wide, axis=-1, keepdims=True)
            grad = g_buf[at].astype(F32) + inv * scaled - h_wide * (inv * inv * inv * proj)
            gs_buf[at] = grad.astype(BF16)
            dul_buf[at] = grad_u

        @pl.when(lower)
        def _():
            for n in range(group):
                at = chunk * group + n
                send_grad(at, gs_buf[at].astype(F32), gatein_buf, tab_in, dn_buf)
            exchange(4, 2, chunk, dn_buf, dr_buf, lambda k: ahead(k, sec - 1), order_all)
            down(line_g, chunk, sec - 1).start()
            for n in range(group):
                at = chunk * group + n
                slope_of_gates(at)
            down(line_l, chunk, sec - 1).start()

        @pl.when(first)
        def _():
            for target in range(1, ns):
                gin_copy(chunk, target).start()
            gin_ref[span(chunk)] = gs_buf[span(chunk), :, 0:part]

        for n in range(group):
            at = chunk * group + n
            h_wide = h_buf[at].astype(F32)
            acc_g[...] += jnp.sum(dul_buf[at] * h_wide * inv_buf[at][:, :1], axis=0, keepdims=True)

    latest = chunks + LAG - 1
    turn = jnp.minimum(LAG + BETWEEN * (ns - 1 - sec), latest)
    tasks = ((tokens, 0), (experts, LAG), (expert_grads, turn), (grads, turn + LAG))

    def step(i, carry):
        for task, lag in tasks:
            at = i - lag

            @pl.when((at >= 0) & (at < chunks))
            def _():
                task(at)

        return carry

    lax.fori_loop(0, latest + chunks + LAG, step, 0)

    for i in range(ne):
        gain_s[i : i + 1, :] = acc_g[:, i * piece : (i + 1) * piece].astype(BF16)
    for k in order:
        gain_copy(k).start()

    @pl.when(last)
    def _():
        sum_pieces()

    sums = sum_r.at[:, pl.ds(0, (ne - 1) * piece)]
    wait_all(sums, red_recv.at[1])
    results[0].start()
    @pl.when(sec != 0)
    def _():
        def take(chunk, carry):
            dst = gin_r.at[span(chunk)]
            pltpu.make_async_copy(dst, dst, gin_recv.at[chunk]).wait()
            return carry

        lax.fori_loop(0, chunks, take, 0)
        gin_ref[...] = gin_r[...]

    results[1].start()
    gains = gain_r.at[pl.ds(1, ne - 1)]
    wait_all(gains, red_recv.at[2])
    total = gain_s[...].astype(F32)
    for k in range(1, ne):
        total = total + gain_r[k].astype(F32)
    for i in range(ne):
        gain_sum_ref[:, i * piece : (i + 1) * piece] = total[i : i + 1, :]

    results[2].start()

    wait_all(part_r.at[pl.ds(1, ne - 1)], red_send.at[0])
    wait_all(sums, red_send.at[1])
    wait_all(gains, red_send.at[2])
    for store in stores + results:
        store.wait()

    def drain(chunk, carry):
        wait_all(others(xs_buf, chunk), send_sem.at[0, chunk])
        wait_all(others(us_buf, chunk), send_sem.at[3, chunk])

        @pl.when(inner)
        def _():
            wait_all(ys_buf.at[span(chunk)], send_sem.at[1, chunk])
            up(line_h, chunk).wait_send()
            up(line_gate, chunk).wait_send()

        @pl.when(last)
        def _():
            wait_all(other_scalars(sv_buf, chunk), send_sem.at[1, chunk])
            wait_all(others(ds_buf, chunk), send_sem.at[2, chunk])

        @pl.when(lower)
        def _():
            wait_all(dn_buf.at[span(chunk)], send_sem.at[4, chunk])
            down(line_g, chunk).wait_send()
            down(line_l, chunk).wait_send()

        @pl.when(first)
        def _():
            for target in range(1, ns):
                gin_copy(chunk, target).wait_send()

        return carry

    lax.fori_loop(0, chunks, drain, 0)

    @pl.when(sec != 0)
    def _():
        gathers[0].wait_send()
        gathers[1].wait_send()

    @pl.when(sec != ns - 1)
    def _():
        gathers[2].wait_send()
        table_copy(0).wait_send()


def weight_grad_kernel(
    steps, rows_hbm, q_hbm, hid_hbm, dyr_hbm, gin_hbm, router_hbm, gain_hbm,
    gu_hbm, dn_hbm, gin_out, router_out, gain_out,
    rows_ref, q_ref, hid_ref, dyr_ref, gin_ref, router_ref, gain_ref, gu_ref, dn_ref, sem, load_sem, pass_sem,
):
    sources = (rows_hbm, q_hbm, hid_hbm, dyr_hbm, gin_hbm, router_hbm, gain_hbm)
    landings = (rows_ref, q_ref, hid_ref, dyr_ref, gin_ref, router_ref, gain_ref)
    loads = [
        pltpu.make_async_copy(src, dst, load_sem.at[n])
        for n, (src, dst) in enumerate(zip(sources, landings))
    ]
    passes = [
        pltpu.make_async_copy(src, dst, pass_sem.at[n])
        for n, (src, dst) in enumerate(zip(landings[4:], (gin_out, router_out, gain_out)))
    ]
    for load in loads:
        load.start()

    def block(lhs, rhs, out, hbm, first, n):
        size = lhs.shape[1] // n

        def copy(i):
            at = pl.ds(pl.multiple_of(i * size, size), size)
            return pltpu.make_async_copy(out.at[at], hbm.at[at], sem.at[first + i])

        def step(i, carry):
            at = pl.ds(pl.multiple_of(i * size, size), size)
            out[at, :] = dot_tn(lhs[:, at], rhs[...])
            copy(i).start()
            return carry

        lax.fori_loop(0, n, step, 0)
        return copy

    loads[0].wait()
    loads[1].wait()
    gu_copy = block(rows_ref, q_ref, gu_ref, gu_hbm, 0, steps[0])
    for load in loads[2:]:
        load.wait()
    for onward in passes:
        onward.start()
    dn_copy = block(hid_ref, dyr_ref, dn_ref, dn_hbm, steps[0], steps[1])
    for i in range(steps[0]):
        gu_copy(i).wait()
    for i in range(steps[1]):
        dn_copy(i).wait()
    for onward in passes:
        onward.wait()


def local(x_in, cotangent, route_ids, norm_gain, router, w_gate_up, w_down):
    ns, ny, nz = (lax.axis_size(a) for a in ("section", "expert", "dp"))
    micro, tok, part = x_in.shape
    width = part * ns
    ne = ny * nz
    cap = 2 * tok // ne
    cells = ne * cap
    ffw = w_down.shape[2]
    chunks = micro // GROUP
    piece = width // ne
    vmem = pltpu.VMEM
    wire = vmem((micro, cells * width // (2 * LANES), 2 * LANES), BF16)
    rows = vmem((micro, tok, width), BF16)
    dma = pltpu.SemaphoreType.DMA
    stash = (
        ((micro * cells, width), BF16),
        ((micro * cells, 2 * ffw), BF16),
        ((micro * cells, ffw), BF16),
        ((micro * cells, width), BF16),
    )
    scratch = (
        [
            vmem((micro, tok, part), BF16), vmem((micro, tok, part), BF16), vmem((micro, 2, tok), jnp.int32),
            vmem((1, width), F32), vmem((ne, width), BF16), vmem((micro, tok, part), BF16), vmem((1, width), F32),
        ]
        + [vmem((width, 2 * ffw), BF16), vmem((ffw, width), BF16)]
        + [vmem((2 * ffw, width), BF16), vmem((width, ffw), BF16)]
        + [vmem(*entry) for entry in stash]
        + [
            vmem((micro, 2 * tok + cells, LANES), BF16),
            vmem((micro, 2 * tok + cells, LANES), BF16),
            vmem((micro, tok, ne), F32),
        ]
        + [rows] * 5
        + [wire] * 9
        + [
            vmem((micro, 8 * ne, LANES), F32),
            vmem((micro, 8 * ne, LANES), F32),
            vmem((cells, LANES), F32),
            vmem((micro, 2 * tok, width), BF16),
            vmem((micro, tok, LANES), F32),
            vmem((micro, 2 * tok, LANES), F32),
            vmem((micro, 2 * tok, LANES), F32),
            vmem((micro, tok, LANES), F32),
            vmem((micro, tok, LANES), F32),
            vmem((micro * cells, ffw), F32),
            vmem((micro * cells, ffw), F32),
            vmem((micro, tok, width), F32),
            vmem((2, cells * width // (2 * LANES), LANES), F32),
            vmem((ne, width), F32),
            vmem((1, width), F32),
            vmem((ne, width), BF16), vmem((ne, ne, piece), BF16),
            vmem((ne, piece), F32), vmem((ne, width), F32),
            vmem((ne, piece), BF16), vmem((ne, ne, piece), BF16),
            vmem((micro, tok, part), BF16),
            dma((5, chunks)), dma((5, chunks)), dma((4, chunks)), dma((4, chunks)), dma((2,)),
            dma((3,)), dma((3,)), dma((ns, chunks)), dma((chunks,)), dma((3,)), dma((3,)), dma((14,)),
        ]
    )
    small = (
        jax.ShapeDtypeStruct((micro, tok, part), BF16),
        jax.ShapeDtypeStruct((ne, width), F32),
        jax.ShapeDtypeStruct((1, width), F32),
    )
    anywhere = pl.BlockSpec(memory_space=pl.ANY)
    *saved, grad_in, sum_router, sum_gain = pl.pallas_call(
        functools.partial(stack_kernel, (ns, ny, nz, cap)),
        out_shape=tuple(jax.ShapeDtypeStruct(*entry) for entry in stash) + small,
        in_specs=[anywhere] * 7,
        out_specs=[anywhere] * 7,
        scratch_shapes=scratch,
        compiler_params=pltpu.CompilerParams(
            collective_id=0, has_side_effects=True, vmem_limit_bytes=60 * 1024 * 1024,
        ),
    )(
        x_in, cotangent, jnp.transpose(route_ids[0], (0, 2, 1)), norm_gain, router[0].T,
        w_gate_up[0, 0], w_down[0, 0],
    )
    steps = STEPS
    grad_gu, grad_dn, grad_in, sum_router, sum_gain = pl.pallas_call(
        functools.partial(weight_grad_kernel, steps),
        out_shape=(
            jax.ShapeDtypeStruct((width, 2 * ffw), F32),
            jax.ShapeDtypeStruct((ffw, width), F32),
        )
        + small,
        in_specs=[anywhere] * 7,
        out_specs=[anywhere] * 5,
        scratch_shapes=[vmem(*entry) for entry in stash]
        + [vmem(entry.shape, entry.dtype) for entry in small]
        + [
            vmem((width, 2 * ffw), F32),
            vmem((ffw, width), F32),
            dma((sum(steps),)),
            dma((7,)),
            dma((3,)),
        ],
        compiler_params=pltpu.CompilerParams(vmem_limit_bytes=60 * 1024 * 1024),
    )(*saved, grad_in, sum_router, sum_gain)
    return grad_in, grad_gu[None, None], grad_dn[None, None], sum_router.T[None], sum_gain


def solution(mesh):
    in_specs = (
        P(None, ("expert", "dp"), "section"),
        P(None, ("expert", "dp"), "section"),
        P("section", None, ("expert", "dp"), None),
        P("section", None),
        P("section", None, None),
        P("section", ("expert", "dp"), None, None),
        P("section", ("expert", "dp"), None, None),
    )
    out_specs = (
        P(None, ("expert", "dp"), "section"),
        P("section", ("expert", "dp"), None, None),
        P("section", ("expert", "dp"), None, None),
        P("section", None, None),
        P("section", None),
    )
    return jax.shard_map(local, mesh=mesh, in_specs=in_specs, out_specs=out_specs, check_vma=False)
```

```python
import functools

import jax
import jax.numpy as jnp
from jax import lax
from jax.experimental import pallas as pl
from jax.experimental.pallas import tpu as pltpu
from jax.sharding import PartitionSpec as P

EPS = 1e-05
GROUP = 1
LAG = 1
BETWEEN = 6
STEPS = (8, 4)
LANES = 128
MESH = pl.DeviceIdType.MESH
F32 = jnp.float32
BF16 = jnp.bfloat16


def dot(lhs, rhs):
    return jnp.dot(lhs, rhs, preferred_element_type=F32)


def dot_nt(lhs, rhs):
    return lax.dot_general(lhs, rhs, (((1,), (1,)), ((), ())), preferred_element_type=F32)


def dot_tn(lhs, rhs):
    return lax.dot_general(lhs, rhs, (((0,), (0,)), ((), ())), preferred_element_type=F32)


def stack_kernel(
    sizes,
    x_hbm, cot_hbm, route_hbm, gain_hbm, router_hbm, wgu_hbm, wdn_hbm,
    rows_hbm, q_hbm, hid_hbm, dyr_hbm, gin_hbm, router_sum_hbm, gain_sum_hbm,
    x_ref, cot_ref, route_ref, gain_ref, router_ref, gin_ref, gain_sum_ref,
    wgu_ref, wdn_ref, wgu_t, wdn_t, rows_ref, q_ref, hid_ref, dyr_ref, tab, tab_in, sign_ref,
    h_buf, hin_buf, g_buf, u_buf, gs_buf,
    xs_buf, xr_buf, ys_buf, yr_buf, ds_buf, dn_buf, dr_buf, us_buf, ur_buf,
    sv_buf, sr_buf, cell_buf, pick_buf, inv_buf, gate_buf, gatein_buf, l_buf, ls_buf, slope_buf, silu_buf, dul_buf, wide,
    cols_buf, acc_g, part_s, part_r, sum_s, sum_r, gain_s, gain_r, gin_r,
    send_sem, recv_sem, line_send, line_recv, tab_sem, gather_send, gather_recv, gin_send, gin_recv,
    red_send, red_recv, local_sem,
):
    ns, ny, nz, cap = sizes
    ne = ny * nz
    micro, tok, width = h_buf.shape
    part = width // ns
    cells = ne * cap
    blk = cap * (width // (2 * LANES))
    folds = width // (2 * LANES)
    group = GROUP
    chunks = micro // group
    ffw = wdn_ref.shape[0]
    sec = lax.axis_index("section")
    ey = lax.axis_index("expert")
    ez = lax.axis_index("dp")

    first, last = sec == 0, sec == ns - 1
    inner, lower = sec != ns - 1, sec != 0

    def ahead(k, section=None):
        there = {"expert": lax.rem(ey + k // nz, ny), "dp": lax.rem(ez + k % nz, nz)}
        return there if section is None else {"section": section, **there}

    def behind(k, section=None):
        there = {"expert": lax.rem(ey + ny - k // nz, ny), "dp": lax.rem(ez + nz - k % nz, nz)}
        return there if section is None else {"section": section, **there}

    def far(k):
        ky, kz = k // nz, k % nz
        return min(ky, ny - ky) + min(kz, nz - kz)

    order = sorted(range(1, ne), key=lambda k: -far(k))
    order_all = order + [0]

    loads = [
        pltpu.make_async_copy(src, dst, local_sem.at[n])
        for n, (src, dst) in enumerate(((wgu_hbm, wgu_ref), (wdn_hbm, wdn_ref)))
    ]
    smalls = [
        pltpu.make_async_copy(src, dst, local_sem.at[6 + n])
        for n, (src, dst) in enumerate(
            (
                (x_hbm, x_ref), (cot_hbm, cot_ref), (route_hbm, route_ref),
                (gain_hbm, gain_ref), (router_hbm, router_ref),
            )
        )
    ]
    results = [
        pltpu.make_async_copy(src, dst, local_sem.at[11 + n])
        for n, (src, dst) in enumerate(
            ((sum_r, router_sum_hbm), (gin_ref, gin_hbm), (gain_sum_ref, gain_sum_hbm))
        )
    ]
    stores = [
        pltpu.make_async_copy(src, dst, local_sem.at[2 + n])
        for n, (src, dst) in enumerate(
            ((rows_ref, rows_hbm), (hid_ref, hid_hbm), (dyr_ref, dyr_hbm), (q_ref, q_hbm))
        )
    ]
    for load in smalls + loads:
        load.start()

    barrier = pltpu.get_barrier_semaphore()
    for k in range(1, ne):
        pl.semaphore_signal(barrier, inc=1, device_id=ahead(k), device_id_type=MESH)
        for step in (1, ns - 1):
            there = ahead(k, lax.rem(sec + step, ns))
            pl.semaphore_signal(barrier, inc=1, device_id=there, device_id_type=MESH)
    for step in range(1, ns):
        pl.semaphore_signal(
            barrier, inc=1, device_id={"section": lax.rem(sec + step, ns)}, device_id_type=MESH
        )
    for load in smalls:
        load.wait()
    pl.semaphore_wait(barrier, 3 * (ne - 1) + ns - 1)

    my_cols = pl.ds(pl.multiple_of(sec * part, LANES), part)

    def gather_copy(which, src, dst, first, count, owner):
        at = pl.ds(first, count)
        return pltpu.make_async_remote_copy(
            src_ref=src.at[at], dst_ref=dst.at[at, :, my_cols],
            send_sem=gather_send.at[which], recv_sem=gather_recv.at[which],
            device_id={"section": owner}, device_id_type=MESH,
        )

    gathers = (
        gather_copy(0, x_ref, h_buf, 0, group, 0),
        gather_copy(1, x_ref, h_buf, group, micro - group, 0),
        gather_copy(2, cot_ref, g_buf, 0, micro, ns - 1),
    )

    @pl.when(sec != 0)
    def _():
        gathers[0].start()
        gathers[1].start()

    @pl.when(sec != ns - 1)
    def _():
        gathers[2].start()

    @pl.when(sec == 0)
    def _():
        h_buf[:, :, 0:part] = x_ref[...]

    @pl.when(sec == ns - 1)
    def _():
        g_buf[:, :, (ns - 1) * part :] = cot_ref[...]

    kinds = lax.broadcasted_iota(jnp.int32, (ne, tok), 0)
    place = jnp.zeros((ne, tok), F32)
    for e in range(ne):
        rel = lax.rem(e // nz + ny - ey, ny) * nz + lax.rem(e % nz + nz - ez, nz)
        place = jnp.where(kinds == e, (rel * cap).astype(F32), place)
    earlier = lax.broadcasted_iota(jnp.int32, (tok, tok), 0)
    earlier = (earlier < lax.broadcasted_iota(jnp.int32, (tok, tok), 1)).astype(BF16)
    cell_ids = lax.broadcasted_iota(jnp.int32, (cells, tok), 0).astype(F32)

    def eye(n):
        rows_id = lax.broadcasted_iota(jnp.int32, (n, n), 0)
        return (rows_id == lax.broadcasted_iota(jnp.int32, (n, n), 1)).astype(BF16)

    def tables(at, carry):
        named = route_ref[at]
        hits = [(kinds == named[k : k + 1, :]).astype(F32) for k in range(2)]
        before = dot((hits[0] + hits[1]).astype(BF16), earlier) + place
        for k in range(2):
            cell = jnp.sum(hits[k] * before, axis=0, keepdims=True)
            tab[at, 2 * tok :, k * tok : (k + 1) * tok] = (cell_ids == cell).astype(BF16)
        turned = dot_nt(eye(2 * tok), tab[at, 2 * tok :, : 2 * tok])
        tab[at, : 2 * tok, :cells] = turned.astype(BF16)
        sign_ref[at] = dot_nt(eye(tok), (hits[0] - hits[1]).astype(BF16))
        return carry

    tab[...] = jnp.zeros_like(tab)
    lax.fori_loop(0, micro, tables, 0)

    def table_copy(target):
        return pltpu.make_async_remote_copy(
            src_ref=tab, dst_ref=tab_in, send_sem=tab_sem.at[0], recv_sem=tab_sem.at[1],
            device_id={"section": target}, device_id_type=MESH,
        )

    @pl.when(inner)
    def _():
        table_copy(sec + 1).start()

    def pick(table, at):
        return table[at, : 2 * tok, :cells]

    def put(table, at):
        return table[at, 2 * tok :, : 2 * tok]

    sv_buf[...] = jnp.zeros_like(sv_buf)
    acc_g[...] = jnp.zeros_like(acc_g)

    def span(chunk):
        return pl.ds(chunk * group, group)

    def exchange(sent, kind, chunk, src, dst, target, blocks):
        for k in blocks:
            rows = pl.ds(k * blk, blk)
            pltpu.make_async_remote_copy(
                src_ref=src.at[span(chunk), rows], dst_ref=dst.at[span(chunk), rows],
                send_sem=send_sem.at[sent, chunk], recv_sem=recv_sem.at[kind, chunk],
                device_id=target(k), device_id_type=MESH,
            ).start()

    def wait_all(ref, sem):
        pltpu.make_async_copy(ref, ref, sem).wait()

    def others(buf, chunk):
        return buf.at[span(chunk), pl.ds(blk, (ne - 1) * blk)]

    def arrived(kind, chunk, dst):
        wait_all(others(dst, chunk), recv_sem.at[kind, chunk])

    def all_arrived(kind, chunk, dst):
        wait_all(dst.at[span(chunk)], recv_sem.at[kind, chunk])

    def fold(value, at, send, recv=None):
        for j in range(folds):
            for half in range(2):
                left = (2 * j + half) * LANES
                wide[half, pl.ds(j, cells, stride=folds), :] = value[:, left : left + LANES]
        for half in range(2):
            cols = slice(half * LANES, (half + 1) * LANES)
            packed = wide[half].astype(BF16)
            send[at, :, cols] = packed
            if recv is not None:
                recv[at, 0:blk, cols] = packed[0:blk]

    def unfold(at, recv):
        for half in range(2):
            wide[half] = recv[at, :, half * LANES : (half + 1) * LANES].astype(F32)
        pieces = [
            wide[half, pl.ds(j, cells, stride=folds), :] for j in range(folds) for half in range(2)
        ]
        return jnp.concatenate(pieces, axis=1).astype(BF16)

    def line_copy(way, chunk, src, dst, target):
        return pltpu.make_async_remote_copy(
            src_ref=src.at[span(chunk)], dst_ref=dst.at[span(chunk)],
            send_sem=line_send.at[way, chunk], recv_sem=line_recv.at[way, chunk],
            device_id={"section": target}, device_id_type=MESH,
        )

    def inv_rms(h_wide):
        return lax.rsqrt(jnp.mean(h_wide * h_wide, axis=-1, keepdims=True) + EPS)

    def wait_gather(which, dst, first, count):
        part_ref = dst.at[pl.ds(first, count), :, pl.ds(0, (ns - 1) * part)]
        pltpu.make_async_copy(part_ref, part_ref, gather_recv.at[which]).wait()

    line_h, line_gate, line_g, line_l = range(4)

    def up(way, chunk, target=0):
        pair = (h_buf, hin_buf) if way == line_h else (gate_buf, gatein_buf)
        return line_copy(way, chunk, *pair, target)

    def down(way, chunk, target=0):
        pair = (gs_buf, g_buf) if way == line_g else (ls_buf, l_buf)
        return line_copy(way, chunk, *pair, target)

    def turn_weights():
        for src, dst in ((wgu_ref, wgu_t), (wdn_ref, wdn_t)):
            size = min(2 * LANES, src.shape[1])
            one = eye(size)

            def turn(j, carry, src=src, dst=dst, size=size, one=one):
                at = pl.ds(pl.multiple_of(j * size, size), size)
                dst[at, :] = dot_nt(one, src[:, at]).astype(BF16)
                return carry

            lax.fori_loop(0, src.shape[1] // size, turn, 0)

    for load in loads:
        load.wait()

    @pl.when(sec >= ns // 2)
    def _():
        turn_weights()

    def tokens(chunk):
        @pl.when(first & (chunk == 0))
        def _():
            wait_gather(0, h_buf, 0, group)

        @pl.when(first & (chunk == 1))
        def _():
            wait_gather(1, h_buf, group, micro - group)

        @pl.when(lower & (chunk == 0))
        def _():
            table_copy(0).wait_recv()

        @pl.when(lower)
        def _():
            up(line_h, chunk).wait_recv()
            up(line_gate, chunk).wait_recv()
            all_arrived(1, chunk, yr_buf)
            for n in range(group):
                at = chunk * group + n
                picked = dot(pick(tab_in, at), unfold(at, yr_buf))
                gates = gatein_buf[at][:, :1]
                total = gates[:tok] * picked[:tok] + gates[tok:] * picked[tok:]
                h_buf[at] = (hin_buf[at].astype(F32) + total).astype(BF16)
                pick_buf[at] = picked.astype(BF16)

        for n in range(group):
            at = chunk * group + n
            h_wide = h_buf[at].astype(F32)
            inv = inv_rms(h_wide)
            normed = (h_wide * inv * gain_ref[...]).astype(BF16)
            inv_buf[at] = jnp.broadcast_to(inv, (tok, LANES))
            u_buf[at] = normed
            both = jnp.concatenate([normed, normed], axis=0)
            fold(dot(put(tab, at), both), at, xs_buf, xr_buf)
        exchange(0, 0, chunk, xs_buf, xr_buf, ahead, order)
        for n in range(group):
            at = chunk * group + n
            logits = dot_nt(u_buf[at], router_ref[...])
            gap = jnp.sum(logits * sign_ref[at], axis=-1, keepdims=True)
            gates = jnp.concatenate([jax.nn.sigmoid(gap), jax.nn.sigmoid(-gap)], axis=0)
            gate_buf[at] = jnp.broadcast_to(gates, (2 * tok, LANES))

        @pl.when(inner)
        def _():
            up(line_h, chunk, sec + 1).start()
            up(line_gate, chunk, sec + 1).start()

        @pl.when(last & (chunk == 0))
        def _():
            wait_gather(2, g_buf, 0, micro)

        @pl.when(last)
        def _():
            for n in range(group):
                at = chunk * group + n
                send_grad(at, g_buf[at].astype(F32), gate_buf, tab, ds_buf, dr_buf)
            exchange(2, 2, chunk, ds_buf, dr_buf, ahead, order)

    def send_grad(at, grad, gate_ref, table, send, recv=None):
        scaled = (jnp.concatenate([grad, grad], axis=0) * gate_ref[at][:, :1]).astype(BF16)
        fold(dot(put(table, at), scaled), at, send, recv)

    def experts(chunk):
        arrived(0, chunk, xr_buf)
        rows = pl.ds(pl.multiple_of(chunk * group * cells, cells), group * cells)
        for n in range(group):
            at = chunk * group + n
            rows_ref[pl.ds(pl.multiple_of(at * cells, cells), cells), :] = unfold(at, xr_buf)
        gate_up = dot(rows_ref[rows, :], wgu_ref[...])
        gate_part = gate_up[:, :ffw]
        up_part = gate_up[:, ffw:]
        sig = jax.nn.sigmoid(gate_part)
        silu = gate_part * sig
        hidden = (silu * up_part).astype(BF16)
        hid_ref[rows, :] = hidden

        @pl.when(inner)
        def _():
            out = dot(hid_ref[rows, :], wdn_ref[...])
            for n in range(group):
                fold(out[n * cells : (n + 1) * cells], chunk * group + n, ys_buf)
            exchange(1, 1, chunk, ys_buf, yr_buf, lambda k: behind(k, sec + 1), order_all)

        silu_buf[rows, :] = silu
        slope_buf[rows, :] = up_part * (sig * (1.0 + gate_part * (1.0 - sig)))

        @pl.when(chunk == chunks - 1)
        def _():
            stores[0].start()
            stores[1].start()

        @pl.when((chunk == chunks - 1) & (sec < ns // 2))
        def _():
            turn_weights()

    piece = width // ne
    me = ey * nz + ez
    my_piece = pl.ds(pl.multiple_of(me * piece, LANES), piece)

    def part_copy(k):
        there = lax.rem(ey + k // nz, ny) * nz + lax.rem(ez + k % nz, nz)
        return pltpu.make_async_remote_copy(
            src_ref=part_s.at[:, pl.ds(pl.multiple_of(there * piece, LANES), piece)],
            dst_ref=part_r.at[k], send_sem=red_send.at[0], recv_sem=red_recv.at[0],
            device_id=ahead(k), device_id_type=MESH,
        )

    def sum_copy(k):
        return pltpu.make_async_remote_copy(
            src_ref=sum_s, dst_ref=sum_r.at[:, my_piece],
            send_sem=red_send.at[1], recv_sem=red_recv.at[1],
            device_id=ahead(k), device_id_type=MESH,
        )

    def gain_copy(k):
        return pltpu.make_async_remote_copy(
            src_ref=gain_s, dst_ref=gain_r.at[k],
            send_sem=red_send.at[2], recv_sem=red_recv.at[2],
            device_id=ahead(k), device_id_type=MESH,
        )

    def slope_of_gates(at):
        picked = pick_buf[at].astype(F32)
        gates = gatein_buf[at][:, :1]
        grad = gs_buf[at].astype(F32)
        diff = jnp.sum(grad * (picked[:tok] - picked[tok:]), axis=-1, keepdims=True)
        ls_buf[at] = jnp.broadcast_to(gates[:tok] * gates[tok:] * diff, (tok, LANES))

    def route_grads(chunk):
        for n in range(group):
            at = chunk * group + n
            cols = (l_buf[at][:, :1] * sign_ref[at]).astype(BF16)
            dul_buf[at] = dot(cols, router_ref[...])
            cols_buf[at] = cols

        @pl.when(chunk == chunks - 1)
        def _():
            all_cols = cols_buf[...].reshape(micro * tok, ne)
            total = dot_tn(all_cols, u_buf[...].reshape(micro * tok, width))
            part_s[...] = total.astype(BF16)
            for k in order:
                part_copy(k).start()

    def sum_pieces():
        wait_all(part_r.at[pl.ds(1, ne - 1)], red_recv.at[0])
        total = part_s[:, my_piece].astype(F32)
        for k in range(1, ne):
            total = total + part_r[k].astype(F32)
        sum_s[...] = total
        sum_r[:, my_piece] = total
        for k in order:
            sum_copy(k).start()

    def scalar_copy(k, chunk):
        rows = pl.ds(8 * k, 8)
        return pltpu.make_async_remote_copy(
            src_ref=sv_buf.at[span(chunk), rows], dst_ref=sr_buf.at[span(chunk), rows],
            send_sem=send_sem.at[1, chunk], recv_sem=recv_sem.at[4, chunk],
            device_id=behind(k), device_id_type=MESH,
        )

    def other_scalars(buf, chunk):
        return buf.at[span(chunk), pl.ds(8, (ne - 1) * 8)]

    def expert_grads(chunk):
        @pl.when(inner)
        def _():
            all_arrived(2, chunk, dr_buf)

        @pl.when(last)
        def _():
            arrived(2, chunk, dr_buf)

        rows = pl.ds(pl.multiple_of(chunk * group * cells, cells), group * cells)
        for n in range(group):
            at = chunk * group + n
            dyr_ref[pl.ds(pl.multiple_of(at * cells, cells), cells), :] = unfold(at, dr_buf)
        d_hidden = dot(dyr_ref[rows, :], wdn_t[...])

        @pl.when(last)
        def _():
            both = hid_ref[rows, :].astype(F32) * d_hidden
            for n in range(group):
                at = chunk * group + n
                mine = jnp.sum(both[n * cells : (n + 1) * cells], axis=-1, keepdims=True)
                cell_buf[...] = jnp.broadcast_to(mine, (cells, LANES))
                for r in range(cap):
                    sv_buf[at, pl.ds(r, ne, stride=8), :] = cell_buf[pl.ds(r, ne, stride=cap), :]
                sr_buf[at, 0:8] = sv_buf[at, 0:8]
            for k in order:
                scalar_copy(k, chunk).start()

        q_ref[rows, :ffw] = (d_hidden * slope_buf[rows, :]).astype(BF16)
        q_ref[rows, ffw:] = (d_hidden * silu_buf[rows, :]).astype(BF16)
        out = dot(q_ref[rows, :], wgu_t[...])
        for n in range(group):
            fold(out[n * cells : (n + 1) * cells], chunk * group + n, us_buf, ur_buf)
        exchange(3, 3, chunk, us_buf, ur_buf, behind, order)

        @pl.when(chunk == chunks - 1)
        def _():
            stores[2].start()
            stores[3].start()

        @pl.when(inner)
        def _():
            down(line_l, chunk).wait_recv()
            route_grads(chunk)

    def gin_copy(chunk, target):
        return pltpu.make_async_remote_copy(
            src_ref=gs_buf.at[span(chunk), :, pl.ds(target * part, part)],
            dst_ref=gin_r.at[span(chunk)],
            send_sem=gin_send.at[target, chunk], recv_sem=gin_recv.at[chunk],
            device_id={"section": target}, device_id_type=MESH,
        )

    def grads(chunk):
        @pl.when(last)
        def _():
            wait_all(other_scalars(sr_buf, chunk), recv_sem.at[4, chunk])
            for n in range(group):
                at = chunk * group + n
                for r in range(cap):
                    cell_buf[pl.ds(r, ne, stride=cap), :] = sr_buf[at, pl.ds(r, ne, stride=8), :]
                value = cell_buf[...]
                high = value.astype(BF16)
                low = (value - high.astype(F32)).astype(BF16)
                picked = dot(pick(tab, at), high) + dot(pick(tab, at), low)
                gates = gate_buf[at]
                l_buf[at] = gates[tok:] * picked[:tok] - gates[:tok] * picked[tok:]
            route_grads(chunk)

        @pl.when(inner)
        def _():
            down(line_g, chunk).wait_recv()

        @pl.when(inner & (chunk == chunks - 1))
        def _():
            sum_pieces()

        arrived(3, chunk, ur_buf)
        for n in range(group):
            at = chunk * group + n
            picked = dot(pick(tab, at), unfold(at, ur_buf))
            grad_u = picked[:tok] + picked[tok:] + dul_buf[at]
            h_wide = h_buf[at].astype(F32)
            inv = inv_buf[at][:, :1]
            scaled = grad_u * gain_ref[...]
            proj = jnp.mean(scaled * h_wide, axis=-1, keepdims=True)
            grad = g_buf[at].astype(F32) + inv * scaled - h_wide * (inv * inv * inv * proj)
            gs_buf[at] = grad.astype(BF16)
            dul_buf[at] = grad_u

        @pl.when(lower)
        def _():
            for n in range(group):
                at = chunk * group + n
                send_grad(at, gs_buf[at].astype(F32), gatein_buf, tab_in, dn_buf)
            exchange(4, 2, chunk, dn_buf, dr_buf, lambda k: ahead(k, sec - 1), order_all)
            down(line_g, chunk, sec - 1).start()
            for n in range(group):
                at = chunk * group + n
                slope_of_gates(at)
            down(line_l, chunk, sec - 1).start()

        @pl.when(first)
        def _():
            for target in range(1, ns):
                gin_copy(chunk, target).start()
            gin_ref[span(chunk)] = gs_buf[span(chunk), :, 0:part]

        for n in range(group):
            at = chunk * group + n
            h_wide = h_buf[at].astype(F32)
            acc_g[...] += dul_buf[at] * h_wide * inv_buf[at][:, :1]

    latest = chunks + LAG - 1
    turn = jnp.minimum(LAG + BETWEEN * (ns - 1 - sec), latest)
    tasks = ((tokens, 0), (experts, LAG), (expert_grads, turn), (grads, turn + LAG))

    def step(i, carry):
        for task, lag in tasks:
            at = i - lag

            @pl.when((at >= 0) & (at < chunks))
            def _():
                task(at)

        return carry

    lax.fori_loop(0, latest + chunks + LAG, step, 0)

    gain_total = jnp.sum(acc_g[...], axis=0, keepdims=True)
    for i in range(ne):
        gain_s[i : i + 1, :] = gain_total[:, i * piece : (i + 1) * piece].astype(BF16)
    for k in order:
        gain_copy(k).start()

    @pl.when(last)
    def _():
        sum_pieces()

    sums = sum_r.at[:, pl.ds(0, (ne - 1) * piece)]
    wait_all(sums, red_recv.at[1])
    results[0].start()
    @pl.when(sec != 0)
    def _():
        def take(chunk, carry):
            dst = gin_r.at[span(chunk)]
            pltpu.make_async_copy(dst, dst, gin_recv.at[chunk]).wait()
            return carry

        lax.fori_loop(0, chunks, take, 0)
        gin_ref[...] = gin_r[...]

    results[1].start()
    gains = gain_r.at[pl.ds(1, ne - 1)]
    wait_all(gains, red_recv.at[2])
    total = gain_s[...].astype(F32)
    for k in range(1, ne):
        total = total + gain_r[k].astype(F32)
    for i in range(ne):
        gain_sum_ref[:, i * piece : (i + 1) * piece] = total[i : i + 1, :]

    results[2].start()

    wait_all(part_r.at[pl.ds(1, ne - 1)], red_send.at[0])
    wait_all(sums, red_send.at[1])
    wait_all(gains, red_send.at[2])
    for store in stores + results:
        store.wait()

    def drain(chunk, carry):
        wait_all(others(xs_buf, chunk), send_sem.at[0, chunk])
        wait_all(others(us_buf, chunk), send_sem.at[3, chunk])

        @pl.when(inner)
        def _():
            wait_all(ys_buf.at[span(chunk)], send_sem.at[1, chunk])
            up(line_h, chunk).wait_send()
            up(line_gate, chunk).wait_send()

        @pl.when(last)
        def _():
            wait_all(other_scalars(sv_buf, chunk), send_sem.at[1, chunk])
            wait_all(others(ds_buf, chunk), send_sem.at[2, chunk])

        @pl.when(lower)
        def _():
            wait_all(dn_buf.at[span(chunk)], send_sem.at[4, chunk])
            down(line_g, chunk).wait_send()
            down(line_l, chunk).wait_send()

        @pl.when(first)
        def _():
            for target in range(1, ns):
                gin_copy(chunk, target).wait_send()

        return carry

    lax.fori_loop(0, chunks, drain, 0)

    @pl.when(sec != 0)
    def _():
        gathers[0].wait_send()
        gathers[1].wait_send()

    @pl.when(sec != ns - 1)
    def _():
        gathers[2].wait_send()
        table_copy(0).wait_send()


def weight_grad_kernel(
    steps, rows_hbm, q_hbm, hid_hbm, dyr_hbm, gin_hbm, router_hbm, gain_hbm,
    gu_hbm, dn_hbm, gin_out, router_out, gain_out,
    rows_ref, q_ref, hid_ref, dyr_ref, gin_ref, router_ref, gain_ref, gu_ref, dn_ref, sem, load_sem, pass_sem,
):
    sources = (rows_hbm, q_hbm, hid_hbm, dyr_hbm, gin_hbm, router_hbm, gain_hbm)
    landings = (rows_ref, q_ref, hid_ref, dyr_ref, gin_ref, router_ref, gain_ref)
    loads = [
        pltpu.make_async_copy(src, dst, load_sem.at[n])
        for n, (src, dst) in enumerate(zip(sources, landings))
    ]
    passes = [
        pltpu.make_async_copy(src, dst, pass_sem.at[n])
        for n, (src, dst) in enumerate(zip(landings[4:], (gin_out, router_out, gain_out)))
    ]
    for load in loads:
        load.start()

    def block(lhs, rhs, out, hbm, first, n):
        size = lhs.shape[1] // n

        def copy(i):
            at = pl.ds(pl.multiple_of(i * size, size), size)
            return pltpu.make_async_copy(out.at[at], hbm.at[at], sem.at[first + i])

        def step(i, carry):
            at = pl.ds(pl.multiple_of(i * size, size), size)
            out[at, :] = dot_tn(lhs[:, at], rhs[...])
            copy(i).start()
            return carry

        lax.fori_loop(0, n, step, 0)
        return copy

    loads[0].wait()
    loads[1].wait()
    gu_copy = block(rows_ref, q_ref, gu_ref, gu_hbm, 0, steps[0])
    for load in loads[2:]:
        load.wait()
    for onward in passes:
        onward.start()
    dn_copy = block(hid_ref, dyr_ref, dn_ref, dn_hbm, steps[0], steps[1])
    for i in range(steps[0]):
        gu_copy(i).wait()
    for i in range(steps[1]):
        dn_copy(i).wait()
    for onward in passes:
        onward.wait()


def local(x_in, cotangent, route_ids, norm_gain, router, w_gate_up, w_down):
    ns, ny, nz = (lax.axis_size(a) for a in ("section", "expert", "dp"))
    micro, tok, part = x_in.shape
    width = part * ns
    ne = ny * nz
    cap = 2 * tok // ne
    cells = ne * cap
    ffw = w_down.shape[2]
    chunks = micro // GROUP
    piece = width // ne
    vmem = pltpu.VMEM
    wire = vmem((micro, cells * width // (2 * LANES), 2 * LANES), BF16)
    rows = vmem((micro, tok, width), BF16)
    dma = pltpu.SemaphoreType.DMA
    stash = (
        ((micro * cells, width), BF16),
        ((micro * cells, 2 * ffw), BF16),
        ((micro * cells, ffw), BF16),
        ((micro * cells, width), BF16),
    )
    scratch = (
        [
            vmem((micro, tok, part), BF16), vmem((micro, tok, part), BF16), vmem((micro, 2, tok), jnp.int32),
            vmem((1, width), F32), vmem((ne, width), BF16), vmem((micro, tok, part), BF16), vmem((1, width), F32),
        ]
        + [vmem((width, 2 * ffw), BF16), vmem((ffw, width), BF16)]
        + [vmem((2 * ffw, width), BF16), vmem((width, ffw), BF16)]
        + [vmem(*entry) for entry in stash]
        + [
            vmem((micro, 2 * tok + cells, LANES), BF16),
            vmem((micro, 2 * tok + cells, LANES), BF16),
            vmem((micro, tok, ne), F32),
        ]
        + [rows] * 5
        + [wire] * 9
        + [
            vmem((micro, 8 * ne, LANES), F32),
            vmem((micro, 8 * ne, LANES), F32),
            vmem((cells, LANES), F32),
            vmem((micro, 2 * tok, width), BF16),
            vmem((micro, tok, LANES), F32),
            vmem((micro, 2 * tok, LANES), F32),
            vmem((micro, 2 * tok, LANES), F32),
            vmem((micro, tok, LANES), F32),
            vmem((micro, tok, LANES), F32),
            vmem((micro * cells, ffw), F32),
            vmem((micro * cells, ffw), F32),
            vmem((micro, tok, width), F32),
            vmem((2, cells * width // (2 * LANES), LANES), F32),
            vmem((micro, tok, ne), BF16),
            vmem((tok, width), F32),
            vmem((ne, width), BF16), vmem((ne, ne, piece), BF16),
            vmem((ne, piece), F32), vmem((ne, width), F32),
            vmem((ne, piece), BF16), vmem((ne, ne, piece), BF16),
            vmem((micro, tok, part), BF16),
            dma((5, chunks)), dma((5, chunks)), dma((4, chunks)), dma((4, chunks)), dma((2,)),
            dma((3,)), dma((3,)), dma((ns, chunks)), dma((chunks,)), dma((3,)), dma((3,)), dma((14,)),
        ]
    )
    small = (
        jax.ShapeDtypeStruct((micro, tok, part), BF16),
        jax.ShapeDtypeStruct((ne, width), F32),
        jax.ShapeDtypeStruct((1, width), F32),
    )
    anywhere = pl.BlockSpec(memory_space=pl.ANY)
    *saved, grad_in, sum_router, sum_gain = pl.pallas_call(
        functools.partial(stack_kernel, (ns, ny, nz, cap)),
        out_shape=tuple(jax.ShapeDtypeStruct(*entry) for entry in stash) + small,
        in_specs=[anywhere] * 7,
        out_specs=[anywhere] * 7,
        scratch_shapes=scratch,
        compiler_params=pltpu.CompilerParams(
            collective_id=0, has_side_effects=True, vmem_limit_bytes=60 * 1024 * 1024,
        ),
    )(
        x_in, cotangent, jnp.transpose(route_ids[0], (0, 2, 1)), norm_gain, router[0].T,
        w_gate_up[0, 0], w_down[0, 0],
    )
    steps = STEPS
    grad_gu, grad_dn, grad_in, sum_router, sum_gain = pl.pallas_call(
        functools.partial(weight_grad_kernel, steps),
        out_shape=(
            jax.ShapeDtypeStruct((width, 2 * ffw), F32),
            jax.ShapeDtypeStruct((ffw, width), F32),
        )
        + small,
        in_specs=[anywhere] * 7,
        out_specs=[anywhere] * 5,
        scratch_shapes=[vmem(*entry) for entry in stash]
        + [vmem(entry.shape, entry.dtype) for entry in small]
        + [
            vmem((width, 2 * ffw), F32),
            vmem((ffw, width), F32),
            dma((sum(steps),)),
            dma((7,)),
            dma((3,)),
        ],
        compiler_params=pltpu.CompilerParams(vmem_limit_bytes=60 * 1024 * 1024),
    )(*saved, grad_in, sum_router, sum_gain)
    return grad_in, grad_gu[None, None], grad_dn[None, None], sum_router.T[None], sum_gain


def solution(mesh):
    in_specs = (
        P(None, ("expert", "dp"), "section"),
        P(None, ("expert", "dp"), "section"),
        P("section", None, ("expert", "dp"), None),
        P("section", None),
        P("section", None, None),
        P("section", ("expert", "dp"), None, None),
        P("section", ("expert", "dp"), None, None),
    )
    out_specs = (
        P(None, ("expert", "dp"), "section"),
        P("section", ("expert", "dp"), None, None),
        P("section", ("expert", "dp"), None, None),
        P("section", None, None),
        P("section", None),
    )
    return jax.shard_map(local, mesh=mesh, in_specs=in_specs, out_specs=out_specs, check_vma=False)
```
